32 devices in a mesh: seq: 8 (over z, core), dp: 4 (over y, x).
Axes of the slice: x: 2, y: 2, z: 4, core: 2. Of those that a mesh axis runs over, the one named last changes fastest.
Arguments:
- block_input: bfloat16 [4, 1024, 4096], P('dp', 'seq'), may hold values from -8 to 8
- cotangent: bfloat16 [4, 1024, 4096], P('dp', 'seq'), may hold values from -6 to 6
- pool_weight: float32 [4, 4, 4096], P(None, None, 'dp'), may hold values from 0.1 to 0.6
Outputs:
- input_grad: bfloat16 [4, 1024, 4096], P('dp', 'seq')
- weight_grad: float32 [4, 4, 4096], P(None, None, 'dp')
The draws below stay inside these ranges and needn't reach their ends.
All inputs are finite; a program needn't handle non-finite values.
Results may differ from the reference program's by a relative error of at most 0.009.
Values may be sent and summed in bfloat16 or wider, within the bound.
No kernel may reach another device: no remote copies, remote signals or barrier semaphores. Data moves between devices by JAX's collectives and lax.ppermute only.
A program may use at most 64 MiB of HBM per device.

```python
import jax
import jax.numpy as jnp
from jax import lax

D = 4096
HEAD_DIM = 128
POOL = 4
TOKENS = 1024
SEQS = 4


def draw_block_input(key, part):
    base = jnp.clip(jax.random.normal(key, (SEQS, TOKENS, D), jnp.float32), -5.0, 5.0)
    return base.astype(jnp.bfloat16)


def shard_levels(stream_key, dims, cuts, least, high):
    factor_of, own = 1.0, jax.random.fold_in(stream_key, 6)
    for position, shards_of in cuts:
        heights = jnp.exp(jax.random.uniform(jax.random.fold_in(own, position), (shards_of,), jnp.float32, least / len(cuts), high / len(cuts)))
        factor_of = factor_of * jnp.repeat(heights, dims[position] // shards_of).reshape([-1 if axis == position else 1 for axis in range(len(dims))])
    return factor_of


def bell_draw(own_key, shape, spread, bound, cuts=(), dtype=jnp.bfloat16):
    drawn = spread * jax.random.normal(own_key, shape, jnp.float32)
    if cuts:
        drawn = drawn * shard_levels(own_key, shape, cuts, -0.22, 0.18)
    return jnp.clip(drawn, -bound, bound).astype(dtype)


def setup_inputs(seed: int = 0) -> dict:
    key_of = jax.random.split(jax.random.key(seed), 4)
    block_input = draw_block_input(jax.random.fold_in(key_of[3], 71), 0)
    cotangent = bell_draw(key_of[1], (SEQS, TOKENS, D), 1.0, 6.0, ((0, 4), (1, 8)))
    pool_weight = jnp.clip(0.1 + 0.5 * jax.random.uniform(key_of[2], (4, POOL, D), jnp.float32) ** shard_levels(key_of[2], (4, POOL, D), ((2, 4),), -0.2, 0.2), 0.1, 0.6)
    return {"block_input": block_input, "cotangent": cotangent, "pool_weight": pool_weight}


def pool_rows(rows, weight):
    grouped = rows.astype(jnp.float32).reshape(rows.shape[0] // POOL, POOL, rows.shape[1])
    return jnp.einsum('cpd,pd->cd', grouped, weight.astype(jnp.float32))


def coarse(query, keys, values, grads):
    length = query.shape[0]
    shape = (length, query.shape[1] // HEAD_DIM, HEAD_DIM)
    q_full = query.reshape(shape).astype(jnp.float32)
    k_full = keys.reshape(shape).astype(jnp.float32)
    v_full = values.reshape(shape).astype(jnp.float32)
    later = jnp.concatenate([grads[1:], jnp.zeros((1, grads.shape[1]), jnp.bfloat16)], 0)
    d_full = later.reshape(shape).astype(jnp.float32)
    scale = HEAD_DIM ** -0.5
    scores = jnp.einsum('qhd,khd->hqk', q_full, k_full) * scale
    allowed = jnp.arange(length)[:, None] >= jnp.arange(length)[None, :]
    scores = jnp.where(allowed[None], scores, -1e30)
    top = jnp.max(scores, -1, keepdims=True)
    expd = jnp.exp(scores - top)
    probs = expd / jnp.sum(expd, -1, keepdims=True)
    probs_low = lax.optimization_barrier(probs.astype(jnp.bfloat16)).astype(jnp.float32)
    attended = jnp.einsum('hqk,khd->qhd', probs_low, v_full)
    prob_grad = jnp.einsum('qhd,khd->hqk', d_full, v_full)
    delta = jnp.einsum('qhd,qhd->hq', d_full, attended)[..., None]
    score_grad = lax.optimization_barrier((probs * (prob_grad - delta)).astype(jnp.bfloat16)).astype(jnp.float32)
    query_grad = jnp.einsum('hqk,khd->qhd', score_grad, k_full) * scale
    key_grad = jnp.einsum('hqk,qhd->khd', score_grad, q_full) * scale
    value_grad = jnp.einsum('hqk,qhd->khd', probs_low, d_full)
    flat = (length, query.shape[1])
    out_low = attended.reshape(flat).astype(jnp.bfloat16)
    shifted = jnp.concatenate([jnp.zeros((1, flat[1]), jnp.bfloat16), out_low[:-1]], 0)
    return (shifted, query_grad.reshape(flat).astype(jnp.bfloat16),
            key_grad.reshape(flat).astype(jnp.bfloat16), value_grad.reshape(flat).astype(jnp.bfloat16))


def one_sequence(pool_weight, pair):
    inputs, upstream = pair
    rows, width = inputs.shape
    query = pool_rows(inputs, pool_weight[0]).astype(jnp.bfloat16)
    keys = pool_rows(inputs, pool_weight[1]).astype(jnp.bfloat16)
    values = pool_rows(inputs, pool_weight[2]).astype(jnp.bfloat16)
    grads = pool_rows(upstream, pool_weight[3]).astype(jnp.bfloat16)
    shifted, query_grad, key_grad, value_grad = coarse(query, keys, values, grads)
    back = (pool_weight[0][None] * query_grad.astype(jnp.float32)[:, None, :]
            + pool_weight[1][None] * key_grad.astype(jnp.float32)[:, None, :]
            + pool_weight[2][None] * value_grad.astype(jnp.float32)[:, None, :])
    back = back.reshape(rows, width).astype(jnp.bfloat16)
    grouped = inputs.astype(jnp.float32).reshape(rows // POOL, POOL, width)
    upgroup = upstream.astype(jnp.float32).reshape(rows // POOL, POOL, width)
    partial_value = jnp.stack([
        jnp.sum(query_grad.astype(jnp.float32)[:, None, :] * grouped, 0),
        jnp.sum(key_grad.astype(jnp.float32)[:, None, :] * grouped, 0),
        jnp.sum(value_grad.astype(jnp.float32)[:, None, :] * grouped, 0),
        jnp.sum(shifted.astype(jnp.float32)[:, None, :] * upgroup, 0)])
    return back, partial_value


def reference(block_input, cotangent, pool_weight):
    backs, partials = lax.map(lambda pair: one_sequence(pool_weight, pair), (block_input, cotangent))
    return backs, jnp.sum(partials, 0)
```

```python
import functools

import jax
import jax.numpy as jnp
from jax import lax
from jax.experimental import pallas as pl
from jax.experimental.pallas import tpu as pltpu
from jax.sharding import PartitionSpec as P

HEAD_DIM = 128
POOL = 4
BF16 = jnp.bfloat16
F32 = jnp.float32


def dot(a, b, ca, cb):
    return lax.dot_general(a, b, (((ca,), (cb,)), ((), ())), preferred_element_type=F32)


def messages(n):
    nz = n // 2
    steps = sorted(range(nz), key=lambda d: (-min(d, nz - d), d))
    return [(d, c) for d in steps for c in range(2) if (d, c) != (0, 0)]


def target(s, n, message, sign=1):
    nz = n // 2
    step, flip = message
    chip = (s // 2 + (step if sign > 0 else nz - step)) % nz
    core = s % 2
    return 2 * chip + (1 - core if flip else core)


def send(block, n, message):
    pairs = [(s, target(s, n, message)) for s in range(n)]
    return lax.ppermute(block, "seq", pairs)


def interleave_matrix(rows):
    r = jnp.arange(rows)
    token = POOL * (r % (rows // POOL)) + r // (rows // POOL)
    return (token[:, None] == jnp.arange(rows)[None, :]).astype(BF16)


def over_query_blocks(length, body):
    step = min(length, 256)
    if length == step:
        body(0, step)
    else:

        def run(i, carry):
            body(pl.multiple_of(i * step, step), step)
            return carry

        lax.fori_loop(0, length // step, run, 0)


def forward_kernel(n, place, pick, weight, *refs):
    blocks = refs[:n]
    q_ref, k_ref, v_ref, x_ref, p_ref, a_ref = refs[n:]
    length, width = q_ref.shape
    rc = length // n
    w = weight[...]
    sel = pick[...]
    for i in range(n):
        at = pl.ds(pl.multiple_of(place[i] * rc, rc), rc)
        x = dot(sel, blocks[i][...], 1, 0)
        parts = [x[j * rc : (j + 1) * rc] for j in range(POOL)]
        for j in range(POOL):
            x_ref[j, at, :] = parts[j].astype(BF16)
        for t, ref in enumerate((q_ref, k_ref, v_ref)):
            total = parts[0] * w[t * POOL][None, :]
            for j in range(1, POOL):
                total = total + parts[j] * w[t * POOL + j][None, :]
            ref[at, :] = total.astype(BF16)
    scale = HEAD_DIM**-0.5
    for h in range(width // HEAD_DIM):
        cols = slice(h * HEAD_DIM, (h + 1) * HEAD_DIM)

        def body(start, step):
            rows = pl.ds(start, step)
            s = dot(q_ref[rows, cols], k_ref[:, cols], 1, 1) * scale
            qi = lax.broadcasted_iota(jnp.int32, s.shape, 0) + start
            ki = lax.broadcasted_iota(jnp.int32, s.shape, 1)
            s = jnp.where(qi >= ki, s, -1e30)
            e = jnp.exp(s - jnp.max(s, -1, keepdims=True))
            p = e * (1.0 / jnp.sum(e, -1, keepdims=True))
            p_ref[h, rows, :] = p
            a_ref[rows, cols] = dot(p.astype(BF16), v_ref[:, cols], 1, 0)

        over_query_blocks(length, body)


def backward_kernel(n, place, goal, pick, weight, q_ref, k_ref, v_ref, x_ref, p_ref, a_ref, *refs):
    blocks = refs[:n]
    outs = refs[n : 2 * n]
    wg_ref = refs[2 * n]
    y_ref, g_ref, s_ref, qg, kg, vg = refs[2 * n + 1 :]
    length, width = q_ref.shape
    rc = length // n
    w = weight[...]
    sel = pick[...]
    for i in range(n):
        at = pl.ds(pl.multiple_of(place[i] * rc, rc), rc)
        y = dot(sel, blocks[i][...], 1, 0)
        parts = [y[j * rc : (j + 1) * rc] for j in range(POOL)]
        for j in range(POOL):
            y_ref[j, at, :] = parts[j].astype(BF16)
        total = parts[0] * w[3 * POOL][None, :]
        for j in range(1, POOL):
            total = total + parts[j] * w[3 * POOL + j][None, :]
        g_ref[at, :] = total.astype(BF16).astype(F32)
    g_ref[length:, :] = jnp.zeros((8, width), F32)
    s_ref[:8, :] = jnp.zeros((8, width), F32)
    s_ref[8:, :] = a_ref[...]
    scale = HEAD_DIM**-0.5
    many = length > 256
    if many:
        kg[...] = jnp.zeros_like(kg)
        vg[...] = jnp.zeros_like(vg)
    g_ref[:length, :] = g_ref[1 : length + 1, :]
    for h in range(width // HEAD_DIM):
        cols = slice(h * HEAD_DIM, (h + 1) * HEAD_DIM)

        def body(start, step):
            rows = pl.ds(start, step)
            later = g_ref[rows, cols]
            low = later.astype(BF16)
            p = p_ref[h, rows, :]
            pg = dot(low, v_ref[:, cols], 1, 1)
            delta = jnp.sum(later * a_ref[rows, cols], -1, keepdims=True)
            sg = (p * (pg - delta)).astype(BF16)
            qg[rows, cols] = dot(sg, k_ref[:, cols], 1, 0) * scale
            new_k = dot(sg, q_ref[rows, cols], 0, 0) * scale
            new_v = dot(p.astype(BF16), low, 0, 0)
            if many:
                kg[:, cols] += new_k
                vg[:, cols] += new_v
            else:
                kg[:, cols] = new_k
                vg[:, cols] = new_v

        over_query_blocks(length, body)
    for t, ref in enumerate((qg, kg, vg)):
        ref[...] = ref[...].astype(BF16).astype(F32)
        for i in range(n):
            at = pl.ds(pl.multiple_of(goal[i] * rc, rc), rc)
            outs[i][t * rc : (t + 1) * rc, :] = ref[at, :].astype(BF16)
        for j in range(POOL):
            wg_ref[t * POOL + j, :] = jnp.sum(ref[...] * x_ref[j].astype(F32), 0)
    shifted = s_ref[7 : length + 7, :].astype(BF16).astype(F32)
    for j in range(POOL):
        wg_ref[3 * POOL + j, :] = jnp.sum(shifted * y_ref[j].astype(F32), 0)


def spread_kernel(n, place, pick, weight, *refs):
    blocks = refs[:n]
    out = refs[n]
    rc = blocks[0].shape[0] // 3
    width = blocks[0].shape[1]
    sel = pick[...]
    for i in range(n):
        cols = pl.ds(pl.multiple_of(place[i] * width, width), width)
        parts = [blocks[i][t * rc : (t + 1) * rc, :].astype(F32) for t in range(3)]
        made = []
        for j in range(POOL):
            total = parts[0] * weight[j, cols][None, :]
            for t in range(1, 3):
                total = total + parts[t] * weight[t * POOL + j, cols][None, :]
            made.append(total.astype(BF16))
        out[:, cols] = dot(sel, jnp.concatenate(made, 0), 0, 0).astype(BF16)


def call(kernel, n_scalar, n_in, out_shape, scratch=()):
    smem = pl.BlockSpec(memory_space=pltpu.SMEM)
    vmem = pl.BlockSpec(memory_space=pltpu.VMEM)
    many = isinstance(out_shape, (list, tuple))
    return pl.pallas_call(
        kernel,
        out_shape=out_shape,
        in_specs=[smem] * n_scalar + [vmem] * n_in,
        out_specs=[vmem] * len(out_shape) if many else vmem,
        scratch_shapes=list(scratch),
    )


def per_device(n, nd, block_input, cotangent, pool_weight):
    inputs = block_input[0]
    upstream = cotangent[0]
    rows, width = inputs.shape
    wide = width // n
    rc = rows // POOL
    length = rc * n
    heads = wide // HEAD_DIM
    me = lax.axis_index("seq")
    todo = messages(n)
    goals = jnp.stack([me] + [target(me, n, m) for m in todo]).astype(jnp.int32)
    froms = jnp.stack([me] + [target(me, n, m, -1) for m in todo]).astype(jnp.int32)
    pick = interleave_matrix(rows)

    def exchange(array):
        cut = [lax.dynamic_slice(array, (0, g * wide), (rows, wide)) for g in [me] + [target(me, n, m) for m in todo]]
        return [cut[0]] + [send(c, n, m) for c, m in zip(cut[1:], todo)]

    x_blocks = exchange(inputs)
    y_blocks = exchange(upstream)
    weights = lax.all_gather(pool_weight.reshape(4 * POOL, -1), "dp", axis=1, tiled=True)
    own = lax.dynamic_slice(weights, (0, me * wide), (4 * POOL, wide))

    shape = jax.ShapeDtypeStruct
    low = shape((length, wide), BF16)
    state = call(
        functools.partial(forward_kernel, n),
        1,
        2 + n,
        [low, low, low, shape((POOL, length, wide), BF16), shape((heads, length, length), F32), shape((length, wide), F32)],
    )(froms, pick, own, *x_blocks)
    results = call(
        functools.partial(backward_kernel, n),
        2,
        8 + n,
        [shape((3 * rc, wide), BF16)] * n + [shape((4 * POOL, wide), F32)],
        [
            pltpu.VMEM((POOL, length, wide), BF16),
            pltpu.VMEM((length + 8, wide), F32),
            pltpu.VMEM((length + 8, wide), F32),
            pltpu.VMEM((length, wide), F32),
            pltpu.VMEM((length, wide), F32),
            pltpu.VMEM((length, wide), F32),
        ],
    )(froms, goals, pick, own, *state, *y_blocks)
    back = [results[0]] + [send(b, n, m) for b, m in zip(results[1:n], todo)]
    sums = jnp.sum(lax.all_gather(results[n], "dp"), 0)
    spread = lax.all_gather(sums, "seq")
    share = n // nd
    mine = lax.dynamic_slice_in_dim(spread, lax.axis_index("dp") * share, share, 0)
    weight_grad = jnp.swapaxes(mine, 0, 1).reshape(4, POOL, share * wide)
    input_grad = call(functools.partial(spread_kernel, n), 1, 2 + n, shape((rows, width), BF16))(
        froms, pick, weights, *back
    )
    return input_grad[None], weight_grad


def solution(mesh):
    n, nd = mesh.shape["seq"], mesh.shape["dp"]
    if n % 2 or n % nd:
        raise ValueError("unsupported mesh")
    placed = (P("dp", "seq", None), P("dp", "seq", None), P(None, None, "dp"))
    return jax.shard_map(
        functools.partial(per_device, n, nd),
        mesh=mesh,
        in_specs=placed,
        out_specs=(P("dp", "seq", None), P(None, None, "dp")),
        check_vma=False,
    )
```

```python
import functools

import jax
import jax.numpy as jnp
from jax import lax
from jax.experimental import pallas as pl
from jax.experimental.pallas import tpu as pltpu
from jax.sharding import PartitionSpec as P

HEAD_DIM = 128
POOL = 4
BF16 = jnp.bfloat16
F32 = jnp.float32


def dot(a, b, ca, cb):
    return lax.dot_general(a, b, (((ca,), (cb,)), ((), ())), preferred_element_type=F32)


def messages(n):
    nz = n // 2
    steps = sorted(range(nz), key=lambda d: (-min(d, nz - d), d))
    return [(d, c) for d in steps for c in range(2) if (d, c) != (0, 0)]


def target(s, n, message, sign=1):
    nz = n // 2
    step, flip = message
    chip = (s // 2 + (step if sign > 0 else nz - step)) % nz
    core = s % 2
    return 2 * chip + (1 - core if flip else core)


def send(block, n, message):
    pairs = [(s, target(s, n, message)) for s in range(n)]
    return lax.ppermute(block, "seq", pairs)


def interleave_matrix(rows):
    r = jnp.arange(rows)
    token = POOL * (r % (rows // POOL)) + r // (rows // POOL)
    return (token[:, None] == jnp.arange(rows)[None, :]).astype(BF16)


def over_query_blocks(length, body):
    step = min(length, 256)
    if length == step:
        body(0, step)
    else:

        def run(i, carry):
            body(pl.multiple_of(i * step, step), step)
            return carry

        lax.fori_loop(0, length // step, run, 0)


def forward_kernel(n, place, pick, weight, *refs):
    blocks = refs[:n]
    q_ref, k_ref, v_ref, x_ref, p_ref, a_ref = refs[n:]
    length, width = q_ref.shape
    rc = length // n
    w = weight[...]
    sel = pick[...]
    for i in range(n):
        at = pl.ds(pl.multiple_of(place[i] * rc, rc), rc)
        x = dot(sel, blocks[i][...], 1, 0)
        parts = [x[j * rc : (j + 1) * rc] for j in range(POOL)]
        for j in range(POOL):
            x_ref[j, at, :] = parts[j].astype(BF16)
        for t, ref in enumerate((q_ref, k_ref, v_ref)):
            total = parts[0] * w[t * POOL][None, :]
            for j in range(1, POOL):
                total = total + parts[j] * w[t * POOL + j][None, :]
            ref[at, :] = total.astype(BF16)
    scale = HEAD_DIM**-0.5
    for h in range(width // HEAD_DIM):
        cols = slice(h * HEAD_DIM, (h + 1) * HEAD_DIM)

        def body(start, step):
            rows = pl.ds(start, step)
            s = dot(q_ref[rows, cols], k_ref[:, cols], 1, 1) * scale
            qi = lax.broadcasted_iota(jnp.int32, s.shape, 0) + start
            ki = lax.broadcasted_iota(jnp.int32, s.shape, 1)
            s = jnp.where(qi >= ki, s, -1e30)
            e = jnp.exp(s - jnp.max(s, -1, keepdims=True))
            p = e * (1.0 / jnp.sum(e, -1, keepdims=True))
            p_ref[h, rows, :] = p
            a_ref[rows, cols] = dot(p.astype(BF16), v_ref[:, cols], 1, 0)

        over_query_blocks(length, body)


def backward_kernel(n, place, goal, pick, weight, q_ref, k_ref, v_ref, x_ref, p_ref, a_ref, *refs):
    blocks = refs[:n]
    outs = refs[n : 2 * n]
    y_ref, g_ref, s_ref, qg, kg, vg, wg_ref = refs[2 * n :]
    length, width = q_ref.shape
    rc = length // n
    w = weight[...]
    sel = pick[...]
    for i in range(n):
        at = pl.ds(pl.multiple_of(place[i] * rc, rc), rc)
        y = dot(sel, blocks[i][...], 1, 0)
        parts = [y[j * rc : (j + 1) * rc] for j in range(POOL)]
        for j in range(POOL):
            y_ref[j, at, :] = parts[j].astype(BF16)
        total = parts[0] * w[3 * POOL][None, :]
        for j in range(1, POOL):
            total = total + parts[j] * w[3 * POOL + j][None, :]
        g_ref[at, :] = total.astype(BF16).astype(F32)
    g_ref[length:, :] = jnp.zeros((8, width), F32)
    s_ref[:8, :] = jnp.zeros((8, width), F32)
    s_ref[8:, :] = a_ref[...]
    scale = HEAD_DIM**-0.5
    many = length > 256
    if many:
        kg[...] = jnp.zeros_like(kg)
        vg[...] = jnp.zeros_like(vg)
    g_ref[:length, :] = g_ref[1 : length + 1, :]
    for h in range(width // HEAD_DIM):
        cols = slice(h * HEAD_DIM, (h + 1) * HEAD_DIM)

        def body(start, step):
            rows = pl.ds(start, step)
            later = g_ref[rows, cols]
            low = later.astype(BF16)
            p = p_ref[h, rows, :]
            pg = dot(low, v_ref[:, cols], 1, 1)
            delta = jnp.sum(later * a_ref[rows, cols], -1, keepdims=True)
            sg = (p * (pg - delta)).astype(BF16)
            qg[rows, cols] = dot(sg, k_ref[:, cols], 1, 0) * scale
            new_k = dot(sg, q_ref[rows, cols], 0, 0) * scale
            new_v = dot(p.astype(BF16), low, 0, 0)
            if many:
                kg[:, cols] += new_k
                vg[:, cols] += new_v
            else:
                kg[:, cols] = new_k
                vg[:, cols] = new_v

        over_query_blocks(length, body)
    for t, ref in enumerate((qg, kg, vg)):
        ref[...] = ref[...].astype(BF16).astype(F32)
        for i in range(n):
            at = pl.ds(pl.multiple_of(goal[i] * rc, rc), rc)
            outs[i][t * rc : (t + 1) * rc, :] = ref[at, :].astype(BF16)
        for j in range(POOL):
            wg_ref[t * POOL + j, :] = jnp.sum(ref[...] * x_ref[j].astype(F32), 0)
    shifted = s_ref[7 : length + 7, :].astype(BF16).astype(F32)
    for j in range(POOL):
        wg_ref[3 * POOL + j, :] = jnp.sum(shifted * y_ref[j].astype(F32), 0)
    low = wg_ref[...].astype(BF16)
    for i in range(n):
        outs[i][3 * rc :, :] = low


def collect_kernel(n, place, *refs):
    out = refs[n]
    width = refs[0].shape[1]
    share = out.shape[3] // width
    for i in range(n):
        part = refs[i][...].astype(F32)
        cols = pl.ds(pl.multiple_of((place[i] % share) * width, width), width)
        for t in range(4):
            out[place[i] // share, t, :, cols] = part[t * POOL : (t + 1) * POOL]


def spread_kernel(n, place, pick, weight, *refs):
    blocks = refs[:n]
    out = refs[n]
    rc = out.shape[0] // POOL
    width = blocks[0].shape[1]
    sel = pick[...]
    for i in range(n):
        cols = pl.ds(pl.multiple_of(place[i] * width, width), width)
        parts = [blocks[i][t * rc : (t + 1) * rc, :].astype(F32) for t in range(3)]
        made = []
        for j in range(POOL):
            total = parts[0] * weight[j, cols][None, :]
            for t in range(1, 3):
                total = total + parts[t] * weight[t * POOL + j, cols][None, :]
            made.append(total.astype(BF16))
        out[:, cols] = dot(sel, jnp.concatenate(made, 0), 0, 0).astype(BF16)


def call(kernel, n_scalar, n_in, out_shape, scratch=()):
    smem = pl.BlockSpec(memory_space=pltpu.SMEM)
    vmem = pl.BlockSpec(memory_space=pltpu.VMEM)
    many = isinstance(out_shape, (list, tuple))
    return pl.pallas_call(
        kernel,
        out_shape=out_shape,
        in_specs=[smem] * n_scalar + [vmem] * n_in,
        out_specs=[vmem] * len(out_shape) if many else vmem,
        scratch_shapes=list(scratch),
    )


def per_device(n, nd, block_input, cotangent, pool_weight):
    inputs = block_input[0]
    upstream = cotangent[0]
    rows, width = inputs.shape
    wide = width // n
    rc = rows // POOL
    length = rc * n
    heads = wide // HEAD_DIM
    me = lax.axis_index("seq")
    todo = messages(n)
    goals = jnp.stack([me] + [target(me, n, m) for m in todo]).astype(jnp.int32)
    froms = jnp.stack([me] + [target(me, n, m, -1) for m in todo]).astype(jnp.int32)
    pick = interleave_matrix(rows)

    def exchange(array):
        cut = [lax.dynamic_slice(array, (0, g * wide), (rows, wide)) for g in [me] + [target(me, n, m) for m in todo]]
        return [cut[0]] + [send(c, n, m) for c, m in zip(cut[1:], todo)]

    x_blocks = exchange(inputs)
    y_blocks = exchange(upstream)
    weights = lax.all_gather(pool_weight.reshape(4 * POOL, -1), "dp", axis=1, tiled=True)
    own = lax.dynamic_slice(weights, (0, me * wide), (4 * POOL, wide))

    shape = jax.ShapeDtypeStruct
    low = shape((length, wide), BF16)
    state = call(
        functools.partial(forward_kernel, n),
        1,
        2 + n,
        [low, low, low, shape((POOL, length, wide), BF16), shape((heads, length, length), F32), shape((length, wide), F32)],
    )(froms, pick, own, *x_blocks)
    results = call(
        functools.partial(backward_kernel, n),
        2,
        8 + n,
        [shape((3 * rc + 4 * POOL, wide), BF16)] * n,
        [
            pltpu.VMEM((POOL, length, wide), BF16),
            pltpu.VMEM((length + 8, wide), F32),
            pltpu.VMEM((length + 8, wide), F32),
            pltpu.VMEM((length, wide), F32),
            pltpu.VMEM((length, wide), F32),
            pltpu.VMEM((length, wide), F32),
            pltpu.VMEM((4 * POOL, wide), F32),
        ],
    )(froms, goals, pick, own, *state, *y_blocks)
    back = [results[0]] + [send(b, n, m) for b, m in zip(results[1:], todo)]
    tail = pl.BlockSpec((4 * POOL, wide), lambda i: (3 * rc // (4 * POOL), 0))
    whole = pl.pallas_call(
        functools.partial(collect_kernel, n),
        out_shape=shape((nd, 4, POOL, width // nd), F32),
        grid=(1,),
        in_specs=[pl.BlockSpec(memory_space=pltpu.SMEM)] + [tail] * n,
    )(froms, *back)
    col = lax.axis_index("dp")
    weight_grad = lax.dynamic_index_in_dim(whole, col, 0, keepdims=False)
    for k in range(1, nd):
        piece = lax.dynamic_index_in_dim(whole, (col + k) % nd, 0, keepdims=False)
        weight_grad = weight_grad + lax.ppermute(piece, "dp", [(d, (d + k) % nd) for d in range(nd)])
    input_grad = call(functools.partial(spread_kernel, n), 1, 2 + n, shape((rows, width), BF16))(
        froms, pick, weights, *back
    )
    return input_grad[None], weight_grad


def solution(mesh):
    n, nd = mesh.shape["seq"], mesh.shape["dp"]
    if n % 2 or n % nd:
        raise ValueError("unsupported mesh")
    placed = (P("dp", "seq", None), P("dp", "seq", None), P(None, None, "dp"))
    return jax.shard_map(
        functools.partial(per_device, n, nd),
        mesh=mesh,
        in_specs=placed,
        out_specs=(P("dp", "seq", None), P(None, None, "dp")),
        check_vma=False,
    )
```

```python
import functools

import jax
import jax.numpy as jnp
from jax import lax
from jax.experimental import pallas as pl
from jax.experimental.pallas import tpu as pltpu
from jax.sharding import PartitionSpec as P

HEAD_DIM = 128
POOL = 4
KINDS = 4
CHUNKS = 2
BF16 = jnp.bfloat16
F32 = jnp.float32


SMEM = pl.BlockSpec(memory_space=pltpu.SMEM)
VMEM = pl.BlockSpec(memory_space=pltpu.VMEM)
ANY = pl.BlockSpec(memory_space=pl.ANY)


def dot(a, b, ca, cb):
    return lax.dot_general(a, b, (((ca,), (cb,)), ((), ())), preferred_element_type=F32)


def messages(n):
    nz = n // 2
    steps = sorted(range(nz), key=lambda d: (-min(d, nz - d), d))
    return [(d, c) for d in steps for c in range(2) if (d, c) != (0, 0)]


def target(s, n, message, sign=1):
    nz = n // 2
    step, flip = message
    chip = (s // 2 + (step if sign > 0 else nz - step)) % nz
    core = s % 2
    return 2 * chip + (1 - core if flip else core)


def send(block, n, message):
    pairs = [(s, target(s, n, message)) for s in range(n)]
    return lax.ppermute(block, "seq", pairs)


def interleave_matrix(rows):
    r = jnp.arange(rows)
    token = POOL * (r % (rows // POOL)) + r // (rows // POOL)
    return (token[:, None] == jnp.arange(rows)[None, :]).astype(BF16)


def aligned(index, size):
    return pl.ds(pl.multiple_of(index * size, size), size)


def cut_kernel(n, wide, first, goal, x_ref, y_ref, *refs):
    outs, sem = refs[:n], refs[n]
    rows = x_ref.shape[0]
    cw = outs[0].shape[1]
    copies = []
    for i in range(n):
        cols = pl.ds(pl.multiple_of(goal[i] * wide + first, HEAD_DIM), cw)
        for t, ref in enumerate((x_ref, y_ref)):
            copy = pltpu.make_async_copy(ref.at[:, cols], outs[i].at[t * rows : (t + 1) * rows, :], sem.at[2 * i + t])
            copy.start()
            copies.append(copy)
    for copy in copies:
        copy.wait()


def block_kernel(n, rc, first, place, goal, spot, pick, weight, *refs):
    blocks = refs[:n]
    outs = refs[n : 2 * n]
    q_ref, k_ref, v_ref, x_ref, y_ref, g_ref, a_ref, qg, kg, vg, wg_ref = refs[2 * n :]
    length, width = q_ref.shape
    rows = rc * POOL
    w = weight[spot[0], :, pl.ds(pl.multiple_of(spot[1] + first, HEAD_DIM), width)]
    sel = pick[...]
    for i in range(n):
        at = aligned(place[i], rc)
        x = dot(sel, blocks[i][:rows, :], 1, 0)
        y = dot(sel, blocks[i][rows:, :], 1, 0)
        for j in range(POOL):
            x_ref[j, at, :] = x[j * rc : (j + 1) * rc].astype(BF16)
            y_ref[j, at, :] = y[j * rc : (j + 1) * rc].astype(BF16)
        for t, (ref, src) in enumerate(((q_ref, x), (k_ref, x), (v_ref, x), (g_ref, y))):
            total = src[:rc] * w[t * POOL][None, :]
            for j in range(1, POOL):
                total = total + src[j * rc : (j + 1) * rc] * w[t * POOL + j][None, :]
            ref[at, :] = total.astype(BF16).astype(ref.dtype)
    g_ref[length:, :] = jnp.zeros((8, width), F32)
    g_ref[:length, :] = g_ref[1 : length + 1, :]
    a_ref[:8, :] = jnp.zeros((8, width), F32)
    scale = HEAD_DIM**-0.5
    step = min(length, 256)
    many = length > step
    if many:
        kg[...] = jnp.zeros_like(kg)
        vg[...] = jnp.zeros_like(vg)
    for h in range(width // HEAD_DIM):
        cols = slice(h * HEAD_DIM, (h + 1) * HEAD_DIM)

        def body(start):
            at = pl.ds(start, step)
            q, k, v = q_ref[at, cols], k_ref[:, cols], v_ref[:, cols]
            s = dot(q, k, 1, 1) * scale
            qi = lax.broadcasted_iota(jnp.int32, s.shape, 0) + start
            ki = lax.broadcasted_iota(jnp.int32, s.shape, 1)
            s = jnp.where(qi >= ki, s, -1e30)
            e = jnp.exp(s - jnp.max(s, -1, keepdims=True))
            p = e * (1.0 / jnp.sum(e, -1, keepdims=True))
            p_low = p.astype(BF16)
            attended = dot(p_low, v, 1, 0)
            later = g_ref[at, cols]
            low = later.astype(BF16)
            delta = jnp.sum(later * attended, -1, keepdims=True)
            sg = (p * (dot(low, v, 1, 1) - delta)).astype(BF16)
            a_ref[pl.ds(start + 8, step), cols] = attended
            qg[at, cols] = (dot(sg, k, 1, 0) * scale).astype(BF16).astype(F32)
            new_k = dot(sg, q, 0, 0) * scale
            new_v = dot(p_low, low, 0, 0)
            if many:
                kg[:, cols] += new_k
                vg[:, cols] += new_v
            else:
                kg[:, cols] = new_k.astype(BF16).astype(F32)
                vg[:, cols] = new_v.astype(BF16).astype(F32)

        if many:

            def run(i, carry):
                body(pl.multiple_of(i * step, step))
                return carry

            lax.fori_loop(0, length // step, run, 0)
        else:
            body(0)
    if many:
        kg[...] = kg[...].astype(BF16).astype(F32)
        vg[...] = vg[...].astype(BF16).astype(F32)
    for t, ref in enumerate((qg, kg, vg)):
        for i in range(n):
            outs[i][t * rc : (t + 1) * rc, :] = ref[aligned(goal[i], rc), :].astype(BF16)
        for j in range(POOL):
            wg_ref[t * POOL + j, :] = jnp.sum(ref[...] * x_ref[j].astype(F32), 0)
    shifted = a_ref[7 : length + 7, :].astype(BF16).astype(F32)
    for j in range(POOL):
        wg_ref[3 * POOL + j, :] = jnp.sum(shifted * y_ref[j].astype(F32), 0)
    low = wg_ref[...].astype(BF16)
    for i in range(n):
        outs[i][3 * rc :, :] = low


def collect_kernel(n, wide, place, *refs):
    blocks, out = refs[:-1], refs[-1]
    cw = blocks[0].shape[1]
    share = out.shape[3] // wide
    for c in range(len(blocks) // n):
        for i in range(n):
            part = blocks[c * n + i][...].astype(F32)
            cols = pl.ds(pl.multiple_of((place[i] % share) * wide + c * cw, HEAD_DIM), cw)
            for t in range(KINDS):
                out[place[i] // share, t, :, cols] = part[t * POOL : (t + 1) * POOL]


def spread_kernel(n, wide, place, part_of, pick, weight, *refs):
    blocks, out = refs[:-1], refs[-1]
    rc = out.shape[0] // POOL
    cw = blocks[0].shape[1]
    share = weight.shape[2] // wide
    sel = pick[...]
    for c in range(len(blocks) // n):
        for i in range(n):
            ref = blocks[c * n + i]
            cols = pl.ds(pl.multiple_of(place[i] * wide + c * cw, HEAD_DIM), cw)
            w = weight[part_of[i], :, pl.ds(pl.multiple_of((place[i] % share) * wide + c * cw, HEAD_DIM), cw)]
            parts = [ref[t * rc : (t + 1) * rc, :].astype(F32) for t in range(3)]
            made = []
            for j in range(POOL):
                total = parts[0] * w[j][None, :]
                for t in range(1, 3):
                    total = total + parts[t] * w[t * POOL + j][None, :]
                made.append(total.astype(BF16))
            out[:, cols] = dot(sel, jnp.concatenate(made, 0), 0, 0).astype(BF16)


def per_device(n, nd, block_input, cotangent, pool_weight):
    inputs = block_input[0]
    upstream = cotangent[0]
    rows, width = inputs.shape
    wide = width // n
    rc = rows // POOL
    length = rc * n
    heads = wide // HEAD_DIM
    chunks = CHUNKS if heads % CHUNKS == 0 else 1
    cw = wide // chunks
    share = n // nd
    me = lax.axis_index("seq")
    col = lax.axis_index("dp")
    todo = messages(n)
    goals = jnp.stack([me] + [target(me, n, m) for m in todo]).astype(jnp.int32)
    froms = jnp.stack([me] + [target(me, n, m, -1) for m in todo]).astype(jnp.int32)
    part_of = ((col - froms // share) % nd).astype(jnp.int32)
    spot = jnp.stack([(col - me // share) % nd, (me % share) * wide]).astype(jnp.int32)
    pick = interleave_matrix(rows)
    shape = jax.ShapeDtypeStruct

    arrived = []
    for c in range(chunks):
        cut = pl.pallas_call(
            functools.partial(cut_kernel, n, wide, c * cw),
            out_shape=[shape((2 * rows, cw), BF16)] * n,
            in_specs=[SMEM, ANY, ANY],
            out_specs=[ANY] * n,
            scratch_shapes=[pltpu.SemaphoreType.DMA((2 * n,))],
        )(goals, inputs, upstream)
        arrived.append([cut[0]] + [send(b, n, m) for b, m in zip(cut[1:], todo)])
        if c == 0:
            own = pool_weight.reshape(KINDS * POOL, -1)
            pieces = [own] + [lax.ppermute(own, "dp", [(d, (d + k) % nd) for d in range(nd)]) for k in range(1, nd)]
            weights = jnp.stack(pieces)

    back = []
    for c in range(chunks):
        full = lambda kind: pltpu.VMEM((length, cw), kind)
        made = pl.pallas_call(
            functools.partial(block_kernel, n, rc, c * cw),
            out_shape=[shape((3 * rc + KINDS * POOL, cw), BF16)] * n,
            in_specs=[SMEM] * 3 + [VMEM] * (2 + n),
            out_specs=[VMEM] * n,
            scratch_shapes=[full(BF16)] * 3
            + [pltpu.VMEM((POOL, length, cw), BF16)] * 2
            + [pltpu.VMEM((length + 8, cw), F32)] * 2
            + [full(F32)] * 3
            + [pltpu.VMEM((KINDS * POOL, cw), F32)],
        )(froms, goals, spot, pick, weights, *arrived[c])
        back += [made[0]] + [send(b, n, m) for b, m in zip(made[1:], todo)]

    tail = pl.BlockSpec((KINDS * POOL, cw), lambda i: (3 * rc // (KINDS * POOL), 0))
    whole = pl.pallas_call(
        functools.partial(collect_kernel, n, wide),
        out_shape=shape((nd, KINDS, POOL, width // nd), F32),
        grid=(1,),
        in_specs=[SMEM] + [tail] * len(back),
    )(froms, *back)
    weight_grad = lax.dynamic_index_in_dim(whole, col, 0, keepdims=False)
    for k in range(1, nd):
        piece = lax.dynamic_index_in_dim(whole, (col + k) % nd, 0, keepdims=False)
        weight_grad = weight_grad + lax.ppermute(piece, "dp", [(d, (d + k) % nd) for d in range(nd)])
    input_grad = pl.pallas_call(
        functools.partial(spread_kernel, n, wide),
        out_shape=shape((rows, width), BF16),
        in_specs=[SMEM] * 2 + [VMEM] * (2 + len(back)),
        out_specs=VMEM,
    )(froms, part_of, pick, weights, *back)
    return input_grad[None], weight_grad


def solution(mesh):
    n, nd = mesh.shape["seq"], mesh.shape["dp"]
    if n % 2 or n % nd:
        raise ValueError("unsupported mesh")
    placed = (P("dp", "seq", None), P("dp", "seq", None), P(None, None, "dp"))
    return jax.shard_map(
        functools.partial(per_device, n, nd),
        mesh=mesh,
        in_specs=placed,
        out_specs=(P("dp", "seq", None), P(None, None, "dp")),
        check_vma=False,
    )
```

```python
import functools

import jax
import jax.numpy as jnp
from jax import lax
from jax.experimental import pallas as pl
from jax.experimental.pallas import tpu as pltpu
from jax.sharding import PartitionSpec as P


HEAD_DIM = 128
POOL = 4
KINDS = 4
CHUNKS = 2
BF16 = jnp.bfloat16
F32 = jnp.float32


VMEM = pl.BlockSpec(memory_space=pltpu.VMEM)
ANY = pl.BlockSpec(memory_space=pl.ANY)


def dot(a, b, ca, cb):
    return lax.dot_general(a, b, (((ca,), (cb,)), ((), ())), preferred_element_type=F32)


def messages(n):
    nz = n // 2
    steps = sorted(range(nz), key=lambda d: (-min(d, nz - d), d))
    return [(d, c) for d in steps for c in range(2) if (d, c) != (0, 0)]


def target(s, n, message, sign=1):
    nz = n // 2
    step, flip = message
    if isinstance(s, int):
        half, core = divmod(s, 2)
        chip = (half + (step if sign > 0 else nz - step)) % nz
    else:
        half, core = lax.div(s, 2), lax.rem(s, 2)
        chip = lax.rem(half + (step if sign > 0 else nz - step), nz)
    return 2 * chip + (1 - core if flip else core)


def send(block, n, message):
    pairs = [(s, target(s, n, message)) for s in range(n)]
    return lax.ppermute(block, "seq", pairs)


def places(n, sign=1):
    me = lax.axis_index("seq")
    return [me] + [target(me, n, m, sign) for m in messages(n)]


def interleave_matrix(rows):
    r = lax.broadcasted_iota(jnp.int32, (rows, rows), 0)
    t = lax.broadcasted_iota(jnp.int32, (rows, rows), 1)
    hit = t == POOL * r
    for j in range(1, POOL):
        hit = hit | (t - j == POOL * r - j * rows)
    return jnp.where(hit, 1.0, 0.0).astype(BF16)


def aligned(index, size):
    return pl.ds(pl.multiple_of(index * size, size), size)


def cut_kernel(n, wide, first, x_ref, y_ref, *refs):
    outs, sem = refs[:n], refs[n]
    rows = x_ref.shape[0]
    cw = outs[0].shape[1]
    copies = []
    goal = places(n)
    for i in range(n):
        cols = pl.ds(pl.multiple_of(goal[i] * wide + first, HEAD_DIM), cw)
        for t, ref in enumerate((x_ref, y_ref)):
            copy = pltpu.make_async_copy(ref.at[:, cols], outs[i].at[t * rows : (t + 1) * rows, :], sem.at[2 * i + t])
            copy.start()
            copies.append(copy)
    for copy in copies:
        copy.wait()


def block_kernel(n, nd, rc, wide, first, weight, *refs):
    blocks = refs[:n]
    outs = refs[n : 2 * n]
    q_ref, k_ref, v_ref, x_ref, y_ref, g_ref, a_ref, qg, kg, vg, wg_ref = refs[2 * n :]
    length, width = q_ref.shape
    rows = rc * POOL
    place, goal = places(n, -1), places(n)
    me, col, share = lax.axis_index("seq"), lax.axis_index("dp"), n // nd
    w = weight[
        lax.rem(col - lax.div(me, share) + nd, nd),
        :,
        pl.ds(pl.multiple_of(lax.rem(me, share) * wide + first, HEAD_DIM), width),
    ]
    sel = interleave_matrix(rows)
    for i in range(n):
        at = aligned(place[i], rc)
        x = dot(sel, blocks[i][:rows, :], 1, 0)
        y = dot(sel, blocks[i][rows:, :], 1, 0)
        for j in range(POOL):
            x_ref[j, at, :] = x[j * rc : (j + 1) * rc].astype(BF16)
            y_ref[j, at, :] = y[j * rc : (j + 1) * rc].astype(BF16)
        for t, (ref, src) in enumerate(((q_ref, x), (k_ref, x), (v_ref, x), (g_ref, y))):
            total = src[:rc] * w[t * POOL][None, :]
            for j in range(1, POOL):
                total = total + src[j * rc : (j + 1) * rc] * w[t * POOL + j][None, :]
            ref[at, :] = total.astype(BF16).astype(ref.dtype)
    g_ref[length:, :] = jnp.zeros((8, width), F32)
    g_ref[:length, :] = g_ref[1 : length + 1, :]
    a_ref[:8, :] = jnp.zeros((8, width), F32)
    scale = HEAD_DIM**-0.5
    step = min(length, 256)
    many = length > step
    if many:
        kg[...] = jnp.zeros_like(kg)
        vg[...] = jnp.zeros_like(vg)
    for h in range(width // HEAD_DIM):
        cols = slice(h * HEAD_DIM, (h + 1) * HEAD_DIM)

        def body(start):
            at = pl.ds(start, step)
            q, k, v = q_ref[at, cols], k_ref[:, cols], v_ref[:, cols]
            s = dot(q, k, 1, 1) * scale
            qi = lax.broadcasted_iota(jnp.int32, s.shape, 0) + start
            ki = lax.broadcasted_iota(jnp.int32, s.shape, 1)
            s = jnp.where(qi >= ki, s, -1e30)
            e = jnp.exp(s - jnp.max(s, -1, keepdims=True))
            p = e * (1.0 / jnp.sum(e, -1, keepdims=True))
            p_low = p.astype(BF16)
            attended = dot(p_low, v, 1, 0)
            later = g_ref[at, cols]
            low = later.astype(BF16)
            delta = jnp.sum(later * attended, -1, keepdims=True)
            sg = (p * (dot(low, v, 1, 1) - delta)).astype(BF16)
            a_ref[pl.ds(start + 8, step), cols] = attended
            qg[at, cols] = (dot(sg, k, 1, 0) * scale).astype(BF16).astype(F32)
            new_k = dot(sg, q, 0, 0) * scale
            new_v = dot(p_low, low, 0, 0)
            if many:
                kg[:, cols] += new_k
                vg[:, cols] += new_v
            else:
                kg[:, cols] = new_k.astype(BF16).astype(F32)
                vg[:, cols] = new_v.astype(BF16).astype(F32)

        if many:

            def run(i, carry):
                body(pl.multiple_of(i * step, step))
                return carry

            lax.fori_loop(0, length // step, run, 0)
        else:
            body(0)
    if many:
        kg[...] = kg[...].astype(BF16).astype(F32)
        vg[...] = vg[...].astype(BF16).astype(F32)
    for t, ref in enumerate((qg, kg, vg)):
        for i in range(n):
            outs[i][t * rc : (t + 1) * rc, :] = ref[aligned(goal[i], rc), :].astype(BF16)
        for j in range(POOL):
            wg_ref[t * POOL + j, :] = jnp.sum(ref[...] * x_ref[j].astype(F32), 0)
    shifted = a_ref[7 : length + 7, :].astype(BF16).astype(F32)
    for j in range(POOL):
        wg_ref[3 * POOL + j, :] = jnp.sum(shifted * y_ref[j].astype(F32), 0)
    low = wg_ref[...].astype(BF16)
    for i in range(n):
        outs[i][3 * rc :, :] = low


def collect_kernel(n, nd, wide, *refs):
    blocks, outs, held = refs[: -nd - 1], refs[-nd - 1 : -1], refs[-1]
    place, col, share = places(n, -1), lax.axis_index("dp"), n // nd
    cw = blocks[0].shape[1]
    for c in range(len(blocks) // n):
        for i in range(n):
            part = blocks[c * n + i][...].astype(F32)
            cols = pl.ds(pl.multiple_of(lax.rem(place[i], share) * wide + c * cw, HEAD_DIM), cw)
            for t in range(KINDS):
                held[lax.div(place[i], share), t, :, cols] = part[t * POOL : (t + 1) * POOL]
    for k in range(nd):
        outs[k][...] = held[lax.rem(col + k, nd)]


def spread_kernel(n, nd, wide, weight, *refs):
    blocks, out = refs[:-1], refs[-1]
    place, col, share = places(n, -1), lax.axis_index("dp"), n // nd
    rc = out.shape[0] // POOL
    cw = blocks[0].shape[1]
    sel = interleave_matrix(rc * POOL)
    for c in range(len(blocks) // n):
        for i in range(n):
            ref = blocks[c * n + i]
            cols = pl.ds(pl.multiple_of(place[i] * wide + c * cw, HEAD_DIM), cw)
            w = weight[
                lax.rem(col - lax.div(place[i], share) + nd, nd),
                :,
                pl.ds(pl.multiple_of(lax.rem(place[i], share) * wide + c * cw, HEAD_DIM), cw),
            ]
            parts = [ref[t * rc : (t + 1) * rc, :].astype(F32) for t in range(3)]
            made = []
            for j in range(POOL):
                total = parts[0] * w[j][None, :]
                for t in range(1, 3):
                    total = total + parts[t] * w[t * POOL + j][None, :]
                made.append(total.astype(BF16))
            out[:, cols] = dot(sel, jnp.concatenate(made, 0), 0, 0).astype(BF16)


def per_device(n, nd, block_input, cotangent, pool_weight):
    inputs = block_input[0]
    upstream = cotangent[0]
    rows, width = inputs.shape
    wide = width // n
    rc = rows // POOL
    length = rc * n
    heads = wide // HEAD_DIM
    chunks = CHUNKS if heads % CHUNKS == 0 else 1
    cw = wide // chunks
    todo = messages(n)
    shape = jax.ShapeDtypeStruct

    arrived = []
    for c in range(chunks):
        cut = pl.pallas_call(
            functools.partial(cut_kernel, n, wide, c * cw),
            out_shape=[shape((2 * rows, cw), BF16)] * n,
            in_specs=[ANY, ANY],
            out_specs=[VMEM] * n,
            scratch_shapes=[pltpu.SemaphoreType.DMA((2 * n,))],
        )(inputs, upstream)
        arrived.append([cut[0]] + [send(b, n, m) for b, m in zip(cut[1:], todo)])
    own = pool_weight.reshape(KINDS * POOL, -1)
    pieces = [own] + [lax.ppermute(own, "dp", [(d, (d + k) % nd) for d in range(nd)]) for k in range(1, nd)]
    weights = jnp.stack(pieces)

    back = []
    for c in range(chunks):
        full = lambda kind: pltpu.VMEM((length, cw), kind)
        made = pl.pallas_call(
            functools.partial(block_kernel, n, nd, rc, wide, c * cw),
            out_shape=[shape((3 * rc + KINDS * POOL, cw), BF16)] * n,
            in_specs=[VMEM] * (1 + n),
            out_specs=[VMEM] * n,
            scratch_shapes=[full(BF16)] * 3
            + [pltpu.VMEM((POOL, length, cw), BF16)] * 2
            + [pltpu.VMEM((length + 8, cw), F32)] * 2
            + [full(F32)] * 3
            + [pltpu.VMEM((KINDS * POOL, cw), F32)],
        )(weights, *arrived[c])
        back += [made[0]] + [send(b, n, m) for b, m in zip(made[1:], todo)]

    tail = pl.BlockSpec((KINDS * POOL, cw), lambda i: (3 * rc // (KINDS * POOL), 0))
    owned = (KINDS, POOL, width // nd)
    part = pl.BlockSpec(owned, lambda i: (0, 0, 0))
    shares = pl.pallas_call(
        functools.partial(collect_kernel, n, nd, wide),
        out_shape=[shape(owned, F32)] * nd,
        grid=(1,),
        in_specs=[tail] * len(back),
        out_specs=[part] * nd,
        scratch_shapes=[pltpu.VMEM((nd,) + owned, F32)],
    )(*back)
    weight_grad = shares[0]
    for k in range(1, nd):
        weight_grad = weight_grad + lax.ppermute(shares[k], "dp", [(d, (d + k) % nd) for d in range(nd)])
    input_grad = pl.pallas_call(
        functools.partial(spread_kernel, n, nd, wide),
        out_shape=shape((rows, width), BF16),
        in_specs=[VMEM] * (1 + len(back)),
        out_specs=VMEM,
    )(weights, *back)
    return input_grad[None], weight_grad


def solution(mesh):
    n, nd = mesh.shape["seq"], mesh.shape["dp"]
    if n % 2 or n % nd:
        raise ValueError("unsupported mesh")
    placed = (P("dp", "seq", None), P("dp", "seq", None), P(None, None, "dp"))

    def whole_step(*arrays):
        return per_device(n, nd, *arrays)

    return jax.shard_map(
        whole_step,
        mesh=mesh,
        in_specs=placed,
        out_specs=(P("dp", "seq", None), P(None, None, "dp")),
        check_vma=False,
    )
```

```python
import functools

import jax
import jax.numpy as jnp
from jax import lax
from jax.experimental import pallas as pl
from jax.experimental.pallas import tpu as pltpu
from jax.sharding import PartitionSpec as P


HEAD_DIM = 128
POOL = 4
KINDS = 4
BF16 = jnp.bfloat16
F32 = jnp.float32


VMEM = pl.BlockSpec(memory_space=pltpu.VMEM)
ANY = pl.BlockSpec(memory_space=pl.ANY)


def dot(a, b, ca, cb):
    return lax.dot_general(a, b, (((ca,), (cb,)), ((), ())), preferred_element_type=F32)


def messages(n):
    nz = n // 2
    steps = sorted(range(nz), key=lambda d: (-min(d, nz - d), d))
    return [(d, c) for d in steps for c in range(2) if (d, c) != (0, 0)]


def target(s, n, message, sign=1):
    nz = n // 2
    step, flip = message
    if isinstance(s, int):
        half, core = divmod(s, 2)
        chip = (half + (step if sign > 0 else nz - step)) % nz
    else:
        half, core = lax.div(s, 2), lax.rem(s, 2)
        chip = lax.rem(half + (step if sign > 0 else nz - step), nz)
    return 2 * chip + (1 - core if flip else core)


def send(block, n, message):
    pairs = [(s, target(s, n, message)) for s in range(n)]
    return lax.ppermute(block, "seq", pairs)


def places(n, sign=1):
    me = lax.axis_index("seq")
    return [me] + [target(me, n, m, sign) for m in messages(n)]


def interleave_matrix(rows):
    r = lax.broadcasted_iota(jnp.int32, (rows, rows), 0)
    t = lax.broadcasted_iota(jnp.int32, (rows, rows), 1)
    hit = t == POOL * r
    for j in range(1, POOL):
        hit = hit | (t - j == POOL * r - j * rows)
    return jnp.where(hit, 1.0, 0.0).astype(BF16)


def aligned(index, size):
    return pl.ds(pl.multiple_of(index * size, size), size)


def cut_kernel(n, wide, first, x_ref, y_ref, *refs):
    outs, sem = refs[:n], refs[n]
    rows = x_ref.shape[0]
    cw = outs[0].shape[1]
    copies = []
    goal = places(n)
    for i in range(n):
        cols = pl.ds(pl.multiple_of(goal[i] * wide + first, HEAD_DIM), cw)
        for t, ref in enumerate((x_ref, y_ref)):
            copy = pltpu.make_async_copy(ref.at[:, cols], outs[i].at[t * rows : (t + 1) * rows, :], sem.at[2 * i + t])
            copy.start()
            copies.append(copy)
    for copy in copies:
        copy.wait()


def block_kernel(n, nd, rc, wide, first, weight, *refs):
    blocks = refs[:n]
    outs = refs[n : 2 * n]
    q_ref, k_ref, v_ref, x_ref, y_ref, g_ref, a_ref, qg, kg, vg, wg_ref = refs[2 * n :]
    length, width = q_ref.shape
    rows = rc * POOL
    place, goal = places(n, -1), places(n)
    me, col, share = lax.axis_index("seq"), lax.axis_index("dp"), n // nd
    w = weight[
        lax.rem(col - lax.div(me, share) + nd, nd),
        :,
        pl.ds(pl.multiple_of(lax.rem(me, share) * wide + first, HEAD_DIM), width),
    ]
    sel = interleave_matrix(rows)
    for i in range(n):
        at = aligned(place[i], rc)
        x = dot(sel, blocks[i][:rows, :], 1, 0)
        y = dot(sel, blocks[i][rows:, :], 1, 0)
        for j in range(POOL):
            x_ref[j, at, :] = x[j * rc : (j + 1) * rc].astype(BF16)
            y_ref[j, at, :] = y[j * rc : (j + 1) * rc].astype(BF16)
        for t, (ref, src) in enumerate(((q_ref, x), (k_ref, x), (v_ref, x), (g_ref, y))):
            total = src[:rc] * w[t * POOL][None, :]
            for j in range(1, POOL):
                total = total + src[j * rc : (j + 1) * rc] * w[t * POOL + j][None, :]
            ref[at, :] = total.astype(BF16).astype(ref.dtype)
    g_ref[length:, :] = jnp.zeros((8, width), F32)
    g_ref[:length, :] = g_ref[1 : length + 1, :]
    a_ref[:8, :] = jnp.zeros((8, width), F32)
    scale = HEAD_DIM**-0.5
    step = min(length, 256)
    many = length > step
    if many:
        kg[...] = jnp.zeros_like(kg)
        vg[...] = jnp.zeros_like(vg)
    for h in range(width // HEAD_DIM):
        cols = slice(h * HEAD_DIM, (h + 1) * HEAD_DIM)

        def body(start):
            at = pl.ds(start, step)
            q, k, v = q_ref[at, cols], k_ref[:, cols], v_ref[:, cols]
            s = dot(q, k, 1, 1) * scale
            qi = lax.broadcasted_iota(jnp.int32, s.shape, 0) + start
            ki = lax.broadcasted_iota(jnp.int32, s.shape, 1)
            s = jnp.where(qi >= ki, s, -1e30)
            e = jnp.exp(s - jnp.max(s, -1, keepdims=True))
            p = e * (1.0 / jnp.sum(e, -1, keepdims=True))
            p_low = p.astype(BF16)
            attended = dot(p_low, v, 1, 0)
            later = g_ref[at, cols]
            low = later.astype(BF16)
            delta = jnp.sum(later * attended, -1, keepdims=True)
            sg = (p * (dot(low, v, 1, 1) - delta)).astype(BF16)
            a_ref[pl.ds(start + 8, step), cols] = attended
            qg[at, cols] = (dot(sg, k, 1, 0) * scale).astype(BF16).astype(F32)
            new_k = dot(sg, q, 0, 0) * scale
            new_v = dot(p_low, low, 0, 0)
            if many:
                kg[:, cols] += new_k
                vg[:, cols] += new_v
            else:
                kg[:, cols] = new_k.astype(BF16).astype(F32)
                vg[:, cols] = new_v.astype(BF16).astype(F32)

        if many:

            def run(i, carry):
                body(pl.multiple_of(i * step, step))
                return carry

            lax.fori_loop(0, length // step, run, 0)
        else:
            body(0)
    if many:
        kg[...] = kg[...].astype(BF16).astype(F32)
        vg[...] = vg[...].astype(BF16).astype(F32)
    for t, ref in enumerate((qg, kg, vg)):
        for i in range(n):
            outs[i][t * rc : (t + 1) * rc, :] = ref[aligned(goal[i], rc), :].astype(BF16)
        for j in range(POOL):
            wg_ref[t * POOL + j, :] = jnp.sum(ref[...] * x_ref[j].astype(F32), 0)
    shifted = a_ref[7 : length + 7, :].astype(BF16).astype(F32)
    for j in range(POOL):
        wg_ref[3 * POOL + j, :] = jnp.sum(shifted * y_ref[j].astype(F32), 0)
    low = wg_ref[...].astype(BF16)
    for i in range(n):
        outs[i][3 * rc :, :] = low


def collect_kernel(n, nd, *refs):
    blocks, outs, held = refs[:n], refs[n : n + nd], refs[n + nd]
    place, col, share = places(n, -1), lax.axis_index("dp"), n // nd
    cw = blocks[0].shape[1]
    for i in range(n):
        part = blocks[i][...].astype(F32)
        cols = aligned(lax.rem(place[i], share), cw)
        for t in range(KINDS):
            held[lax.div(place[i], share), t, :, cols] = part[t * POOL : (t + 1) * POOL]
    for k in range(nd):
        outs[k][...] = held[lax.rem(col + k, nd)]


def total_kernel(wide, spans, *refs):
    parts, out = refs[:-1], refs[-1]
    nd = len(parts) // len(spans)
    for c, (first, cw) in enumerate(spans):
        total = parts[c * nd][...]
        for k in range(1, nd):
            total = total + parts[c * nd + k][...]
        for b in range(total.shape[2] // cw):
            out[:, :, b * wide + first : b * wide + first + cw] = total[:, :, b * cw : (b + 1) * cw]


def spread_kernel(n, nd, wide, first, weight, *refs):
    blocks, (out, made_ref, sem) = refs[:n], refs[-3:]
    place, col, share = places(n, -1), lax.axis_index("dp"), n // nd
    rows, cw = made_ref.shape[1:]
    rc = rows // POOL
    sel = interleave_matrix(rows)
    copies = []
    for i in range(n):
        ref = blocks[i]
        w = weight[
            lax.rem(col - lax.div(place[i], share) + nd, nd),
            :,
            pl.ds(pl.multiple_of(lax.rem(place[i], share) * wide + first, HEAD_DIM), cw),
        ]
        parts = [ref[t * rc : (t + 1) * rc, :].astype(F32) for t in range(3)]
        made = []
        for j in range(POOL):
            total = parts[0] * w[j][None, :]
            for t in range(1, 3):
                total = total + parts[t] * w[t * POOL + j][None, :]
            made.append(total.astype(BF16))
        made_ref[i] = dot(sel, jnp.concatenate(made, 0), 0, 0).astype(BF16)
        cols = pl.ds(pl.multiple_of(place[i] * wide + first, HEAD_DIM), cw)
        copy = pltpu.make_async_copy(made_ref.at[i], out.at[:, cols], sem.at[i])
        copy.start()
        copies.append(copy)
    for copy in copies:
        copy.wait()


def per_device(n, nd, block_input, cotangent, pool_weight):
    inputs = block_input[0]
    upstream = cotangent[0]
    rows, width = inputs.shape
    wide = width // n
    rc = rows // POOL
    length = rc * n
    heads = wide // HEAD_DIM
    share = n // nd
    small = heads // 4
    split = [heads - small, small] if small else [heads]
    spans = [(sum(split[:c]) * HEAD_DIM, h * HEAD_DIM) for c, h in enumerate(split)]
    todo = messages(n)
    shape = jax.ShapeDtypeStruct

    arrived = []
    for first, cw in spans:
        cut = pl.pallas_call(
            functools.partial(cut_kernel, n, wide, first),
            out_shape=[shape((2 * rows, cw), BF16)] * n,
            in_specs=[ANY, ANY],
            out_specs=[VMEM] * n,
            scratch_shapes=[pltpu.SemaphoreType.DMA((2 * n,))],
        )(inputs, upstream)
        arrived.append([cut[0]] + [send(b, n, m) for b, m in zip(cut[1:], todo)])
    own = pool_weight.reshape(KINDS * POOL, -1)
    pieces = [own] + [lax.ppermute(own, "dp", [(d, (d + k) % nd) for d in range(nd)]) for k in range(1, nd)]
    weights = jnp.stack(pieces)

    back = []
    for c, (first, cw) in enumerate(spans):
        full = lambda kind: pltpu.VMEM((length, cw), kind)
        made = pl.pallas_call(
            functools.partial(block_kernel, n, nd, rc, wide, first),
            out_shape=[shape((3 * rc + KINDS * POOL, cw), BF16)] * n,
            in_specs=[VMEM] * (1 + n),
            out_specs=[VMEM] * n,
            scratch_shapes=[full(BF16)] * 3
            + [pltpu.VMEM((POOL, length, cw), BF16)] * 2
            + [pltpu.VMEM((length + 8, cw), F32)] * 2
            + [full(F32)] * 3
            + [pltpu.VMEM((KINDS * POOL, cw), F32)],
        )(weights, *arrived[c])
        back.append([made[0]] + [send(b, n, m) for b, m in zip(made[1:], todo)])

    parts = []
    input_grad = ()
    for c, (first, cw) in enumerate(spans):
        owned = (KINDS, POOL, share * cw)
        shares = pl.pallas_call(
            functools.partial(collect_kernel, n, nd),
            out_shape=[shape(owned, F32)] * nd,
            grid=(1,),
            in_specs=[pl.BlockSpec((KINDS * POOL, cw), lambda i: (3 * rc // (KINDS * POOL), 0))] * n,
            out_specs=[pl.BlockSpec(owned, lambda i: (0, 0, 0))] * nd,
            scratch_shapes=[pltpu.VMEM((nd,) + owned, F32)],
        )(*back[c])
        parts.append(shares[0])
        for k in range(1, nd):
            parts.append(lax.ppermute(shares[k], "dp", [(d, (d + k) % nd) for d in range(nd)]))
        input_grad = (
            pl.pallas_call(
                functools.partial(spread_kernel, n, nd, wide, first),
                out_shape=shape((rows, width), BF16),
                in_specs=[VMEM] * (1 + n) + [ANY] * len(input_grad),
                out_specs=ANY,
                input_output_aliases={1 + n: 0} if input_grad else {},
                scratch_shapes=[pltpu.VMEM((n, rows, cw), BF16), pltpu.SemaphoreType.DMA((n,))],
            )(weights, *back[c], *input_grad),
        )
    weight_grad = pl.pallas_call(
        functools.partial(total_kernel, wide, spans),
        out_shape=shape((KINDS, POOL, width // nd), F32),
        in_specs=[VMEM] * len(parts),
        out_specs=VMEM,
    )(*parts)
    return input_grad[0][None], weight_grad


def solution(mesh):
    n, nd = mesh.shape["seq"], mesh.shape["dp"]
    if n % 2 or n % nd:
        raise ValueError("unsupported mesh")
    placed = (P("dp", "seq", None), P("dp", "seq", None), P(None, None, "dp"))

    def whole_step(*arrays):
        return per_device(n, nd, *arrays)

    return jax.shard_map(
        whole_step,
        mesh=mesh,
        in_specs=placed,
        out_specs=(P("dp", "seq", None), P(None, None, "dp")),
        check_vma=False,
    )
```

```python
import functools

import jax
import jax.numpy as jnp
from jax import lax
from jax.experimental import pallas as pl
from jax.experimental.pallas import tpu as pltpu
from jax.sharding import PartitionSpec as P


HEAD_DIM = 128
POOL = 4
KINDS = 4
CHUNKS = 2
BF16 = jnp.bfloat16
F32 = jnp.float32


VMEM = pl.BlockSpec(memory_space=pltpu.VMEM)
ANY = pl.BlockSpec(memory_space=pl.ANY)


def dot(a, b, ca, cb):
    return lax.dot_general(a, b, (((ca,), (cb,)), ((), ())), preferred_element_type=F32)


def messages(n):
    return [*range(n // 2, n), *range(2, n // 2), 1]


def send(block, axis, n, message):
    return lax.ppermute(block, axis, [(s, s ^ message) for s in range(n)])


def places(n):
    me = lax.axis_index("seq")
    return [me] + [lax.bitwise_xor(me, jnp.int32(m)) for m in messages(n)]


def interleave_matrix(rows):
    r = lax.broadcasted_iota(jnp.int32, (rows, rows), 0)
    t = lax.broadcasted_iota(jnp.int32, (rows, rows), 1)
    hit = t == POOL * r
    for j in range(1, POOL):
        hit = hit | (t - j == POOL * r - j * rows)
    return jnp.where(hit, 1.0, 0.0).astype(BF16)


def aligned(index, size):
    return pl.ds(pl.multiple_of(index * size, size), size)


def cut_kernel(n, wide, first, x_ref, y_ref, *refs):
    outs, sem = refs[:n], refs[n]
    rows = x_ref.shape[0]
    cw = outs[0].shape[1]
    copies = []
    goal = places(n)
    for i in range(n):
        cols = pl.ds(pl.multiple_of(goal[i] * wide + first, HEAD_DIM), cw)
        for t, ref in enumerate((x_ref, y_ref)):
            copy = pltpu.make_async_copy(ref.at[:, cols], outs[i].at[t * rows : (t + 1) * rows, :], sem.at[2 * i + t])
            copy.start()
            copies.append(copy)
    for copy in copies:
        copy.wait()


def block_kernel(n, nd, rc, wide, first, weight, *refs):
    blocks = refs[:n]
    outs = refs[n : 2 * n]
    q_ref, k_ref, v_ref, x_ref, y_ref, g_ref, a_ref, qg, kg, vg, wg_ref = refs[2 * n :]
    length, width = q_ref.shape
    rows = rc * POOL
    place = places(n)
    goal = place
    me, col, share = lax.axis_index("seq"), lax.axis_index("dp"), n // nd
    w = weight[
        lax.bitwise_xor(col, lax.div(me, share)),
        :,
        pl.ds(pl.multiple_of(lax.rem(me, share) * wide + first, HEAD_DIM), width),
    ]
    sel = interleave_matrix(rows)
    for i in range(n):
        at = aligned(place[i], rc)
        x = dot(sel, blocks[i][:rows, :], 1, 0)
        y = dot(sel, blocks[i][rows:, :], 1, 0)
        for j in range(POOL):
            x_ref[j, at, :] = x[j * rc : (j + 1) * rc].astype(BF16)
            y_ref[j, at, :] = y[j * rc : (j + 1) * rc].astype(BF16)
        for t, (ref, src) in enumerate(((q_ref, x), (k_ref, x), (v_ref, x), (g_ref, y))):
            total = src[:rc] * w[t * POOL][None, :]
            for j in range(1, POOL):
                total = total + src[j * rc : (j + 1) * rc] * w[t * POOL + j][None, :]
            ref[at, :] = total.astype(BF16).astype(ref.dtype)
    g_ref[length:, :] = jnp.zeros((8, width), F32)
    g_ref[:length, :] = g_ref[1 : length + 1, :]
    a_ref[:8, :] = jnp.zeros((8, width), F32)
    scale = HEAD_DIM**-0.5
    step = min(length, 256)
    many = length > step
    if many:
        kg[...] = jnp.zeros_like(kg)
        vg[...] = jnp.zeros_like(vg)
    for h in range(width // HEAD_DIM):
        cols = slice(h * HEAD_DIM, (h + 1) * HEAD_DIM)

        def body(start):
            at = pl.ds(start, step)
            q, k, v = q_ref[at, cols], k_ref[:, cols], v_ref[:, cols]
            s = dot(q, k, 1, 1) * scale
            qi = lax.broadcasted_iota(jnp.int32, s.shape, 0) + start
            ki = lax.broadcasted_iota(jnp.int32, s.shape, 1)
            s = jnp.where(qi >= ki, s, -1e30)
            e = jnp.exp(s - jnp.max(s, -1, keepdims=True))
            p = e * (1.0 / jnp.sum(e, -1, keepdims=True))
            p_low = p.astype(BF16)
            attended = dot(p_low, v, 1, 0)
            later = g_ref[at, cols]
            low = later.astype(BF16)
            delta = jnp.sum(later * attended, -1, keepdims=True)
            sg = (p * (dot(low, v, 1, 1) - delta)).astype(BF16)
            a_ref[pl.ds(start + 8, step), cols] = attended
            qg[at, cols] = (dot(sg, k, 1, 0) * scale).astype(BF16).astype(F32)
            new_k = dot(sg, q, 0, 0) * scale
            new_v = dot(p_low, low, 0, 0)
            if many:
                kg[:, cols] += new_k
                vg[:, cols] += new_v
            else:
                kg[:, cols] = new_k.astype(BF16).astype(F32)
                vg[:, cols] = new_v.astype(BF16).astype(F32)

        if many:

            def run(i, carry):
                body(pl.multiple_of(i * step, step))
                return carry

            lax.fori_loop(0, length // step, run, 0)
        else:
            body(0)
    if many:
        kg[...] = kg[...].astype(BF16).astype(F32)
        vg[...] = vg[...].astype(BF16).astype(F32)
    for t, ref in enumerate((qg, kg, vg)):
        for i in range(n):
            outs[i][t * rc : (t + 1) * rc, :] = ref[aligned(goal[i], rc), :].astype(BF16)
        for j in range(POOL):
            wg_ref[t * POOL + j, :] = jnp.sum(ref[...] * x_ref[j].astype(F32), 0)
    shifted = a_ref[7 : length + 7, :].astype(BF16).astype(F32)
    for j in range(POOL):
        wg_ref[3 * POOL + j, :] = jnp.sum(shifted * y_ref[j].astype(F32), 0)
    low = wg_ref[...].astype(BF16)
    for i in range(n):
        outs[i][3 * rc :, :] = low


def collect_kernel(n, nd, wide, *refs):
    blocks, outs, held = refs[: -nd - 1], refs[-nd - 1 : -1], refs[-1]
    place, col, share = places(n), lax.axis_index("dp"), n // nd
    cw = blocks[0].shape[1]
    for c in range(len(blocks) // n):
        for i in range(n):
            part = blocks[c * n + i][...].astype(F32)
            cols = pl.ds(pl.multiple_of(lax.rem(place[i], share) * wide + c * cw, HEAD_DIM), cw)
            for t in range(KINDS):
                held[lax.div(place[i], share), t, :, cols] = part[t * POOL : (t + 1) * POOL]
    for k in range(nd):
        outs[k][...] = held[lax.bitwise_xor(col, jnp.int32(k))]


def spread_kernel(n, nd, wide, weight, *refs):
    blocks, out = refs[:-1], refs[-1]
    place, col, share = places(n), lax.axis_index("dp"), n // nd
    rc = out.shape[0] // POOL
    cw = blocks[0].shape[1]
    sel = interleave_matrix(rc * POOL)
    for c in range(len(blocks) // n):
        for i in range(n):
            ref = blocks[c * n + i]
            cols = pl.ds(pl.multiple_of(place[i] * wide + c * cw, HEAD_DIM), cw)
            w = weight[
                lax.bitwise_xor(col, lax.div(place[i], share)),
                :,
                pl.ds(pl.multiple_of(lax.rem(place[i], share) * wide + c * cw, HEAD_DIM), cw),
            ]
            parts = [ref[t * rc : (t + 1) * rc, :].astype(F32) for t in range(3)]
            made = []
            for j in range(POOL):
                total = parts[0] * w[j][None, :]
                for t in range(1, 3):
                    total = total + parts[t] * w[t * POOL + j][None, :]
                made.append(total.astype(BF16))
            out[:, cols] = dot(sel, jnp.concatenate(made, 0), 0, 0).astype(BF16)


def per_device(n, nd, block_input, cotangent, pool_weight):
    inputs = block_input[0]
    upstream = cotangent[0]
    rows, width = inputs.shape
    wide = width // n
    rc = rows // POOL
    length = rc * n
    heads = wide // HEAD_DIM
    chunks = CHUNKS if heads % CHUNKS == 0 else 1
    cw = wide // chunks
    todo = messages(n)
    shape = jax.ShapeDtypeStruct

    arrived = []
    for c in range(chunks):
        cut = pl.pallas_call(
            functools.partial(cut_kernel, n, wide, c * cw),
            out_shape=[shape((2 * rows, cw), BF16)] * n,
            in_specs=[ANY, ANY],
            out_specs=[VMEM] * n,
            scratch_shapes=[pltpu.SemaphoreType.DMA((2 * n,))],
        )(inputs, upstream)
        arrived.append([cut[0]] + [send(b, "seq", n, m) for b, m in zip(cut[1:], todo)])
    own = pool_weight.reshape(KINDS * POOL, -1)
    pieces = [own] + [send(own, "dp", nd, k) for k in range(1, nd)]
    weights = jnp.stack(pieces)

    back = []
    for c in range(chunks):
        full = lambda kind: pltpu.VMEM((length, cw), kind)
        made = pl.pallas_call(
            functools.partial(block_kernel, n, nd, rc, wide, c * cw),
            out_shape=[shape((3 * rc + KINDS * POOL, cw), BF16)] * n,
            in_specs=[VMEM] * (1 + n),
            out_specs=[VMEM] * n,
            scratch_shapes=[full(BF16)] * 3
            + [pltpu.VMEM((POOL, length, cw), BF16)] * 2
            + [pltpu.VMEM((length + 8, cw), F32)] * 2
            + [full(F32)] * 3
            + [pltpu.VMEM((KINDS * POOL, cw), F32)],
        )(weights, *arrived[c])
        back += [made[0]] + [send(b, "seq", n, m) for b, m in zip(made[1:], todo)]

    tail = pl.BlockSpec((KINDS * POOL, cw), lambda i: (3 * rc // (KINDS * POOL), 0))
    owned = (KINDS, POOL, width // nd)
    part = pl.BlockSpec(owned, lambda i: (0, 0, 0))
    shares = pl.pallas_call(
        functools.partial(collect_kernel, n, nd, wide),
        out_shape=[shape(owned, F32)] * nd,
        grid=(1,),
        in_specs=[tail] * len(back),
        out_specs=[part] * nd,
        scratch_shapes=[pltpu.VMEM((nd,) + owned, F32)],
    )(*back)
    weight_grad = shares[0]
    for k in range(1, nd):
        weight_grad = weight_grad + send(shares[k], "dp", nd, k)
    input_grad = pl.pallas_call(
        functools.partial(spread_kernel, n, nd, wide),
        out_shape=shape((rows, width), BF16),
        in_specs=[VMEM] * (1 + len(back)),
        out_specs=VMEM,
    )(weights, *back)
    return input_grad[None], weight_grad


def solution(mesh):
    n, nd = mesh.shape["seq"], mesh.shape["dp"]
    if n < 4 or n & (n - 1) or n % nd:
        raise ValueError("unsupported mesh")
    placed = (P("dp", "seq", None), P("dp", "seq", None), P(None, None, "dp"))

    def whole_step(*arrays):
        return per_device(n, nd, *arrays)

    return jax.shard_map(
        whole_step,
        mesh=mesh,
        in_specs=placed,
        out_specs=(P("dp", "seq", None), P(None, None, "dp")),
        check_vma=False,
    )
```

```python
import functools

import jax
import jax.numpy as jnp
from jax import lax
from jax.experimental import pallas as pl
from jax.experimental.pallas import tpu as pltpu
from jax.sharding import PartitionSpec as P


HEAD_DIM = 128
POOL = 4
KINDS = 4
CHUNKS = 2
BF16 = jnp.bfloat16
F32 = jnp.float32


VMEM = pl.BlockSpec(memory_space=pltpu.VMEM)
ANY = pl.BlockSpec(memory_space=pl.ANY)


def dot(a, b, ca, cb):
    return lax.dot_general(a, b, (((ca,), (cb,)), ((), ())), preferred_element_type=F32)


def messages(n):
    return [*range(n // 2, n), *range(2, n // 2), 1]


def send(block, axis, n, message):
    return lax.ppermute(block, axis, [(s, s ^ message) for s in range(n)])


def places(n):
    me = lax.axis_index("seq")
    return [me] + [lax.bitwise_xor(me, jnp.int32(m)) for m in messages(n)]


def interleave_matrix(rows):
    r = lax.broadcasted_iota(jnp.int32, (rows, rows), 0)
    t = lax.broadcasted_iota(jnp.int32, (rows, rows), 1)
    hit = t == POOL * r
    for j in range(1, POOL):
        hit = hit | (t - j == POOL * r - j * rows)
    return jnp.where(hit, 1.0, 0.0).astype(BF16)


def aligned(index, size):
    return pl.ds(pl.multiple_of(index * size, size), size)


def cut_kernel(n, wide, first, x_ref, y_ref, *refs):
    outs, sem = refs[:n], refs[n]
    rows = x_ref.shape[0]
    cw = outs[0].shape[1]
    copies = []
    goal = places(n)
    for i in range(n):
        cols = pl.ds(pl.multiple_of(goal[i] * wide + first, HEAD_DIM), cw)
        for t, ref in enumerate((x_ref, y_ref)):
            copy = pltpu.make_async_copy(ref.at[:, cols], outs[i].at[t * rows : (t + 1) * rows, :], sem.at[2 * i + t])
            copy.start()
            copies.append(copy)
    for copy in copies:
        copy.wait()


def block_kernel(n, nd, rc, wide, first, weight, *refs):
    blocks = refs[:n]
    outs = refs[n : 2 * n]
    q_ref, k_ref, v_ref, x_ref, y_ref, g_ref, a_ref, qg, kg, vg, wg_ref = refs[2 * n :]
    length, width = q_ref.shape
    rows = rc * POOL
    place = places(n)
    goal = place
    me, col, share = lax.axis_index("seq"), lax.axis_index("dp"), n // nd
    w = weight[
        lax.bitwise_xor(col, lax.div(me, share)),
        :,
        pl.ds(pl.multiple_of(lax.rem(me, share) * wide + first, HEAD_DIM), width),
    ]
    sel = interleave_matrix(rows)
    for i in range(n):
        at = aligned(place[i], rc)
        x = dot(sel, blocks[i][:rows, :], 1, 0)
        y = dot(sel, blocks[i][rows:, :], 1, 0)
        for j in range(POOL):
            x_ref[j, at, :] = x[j * rc : (j + 1) * rc].astype(BF16)
            y_ref[j, at, :] = y[j * rc : (j + 1) * rc].astype(BF16)
        for t, (ref, src) in enumerate(((q_ref, x), (k_ref, x), (v_ref, x), (g_ref, y))):
            total = src[:rc] * w[t * POOL][None, :]
            for j in range(1, POOL):
                total = total + src[j * rc : (j + 1) * rc] * w[t * POOL + j][None, :]
            ref[at, :] = total.astype(BF16).astype(ref.dtype)
    g_ref[length:, :] = jnp.zeros((8, width), F32)
    g_ref[:length, :] = g_ref[1 : length + 1, :]
    a_ref[:8, :] = jnp.zeros((8, width), F32)
    scale = HEAD_DIM**-0.5
    step = min(length, 256)
    many = length > step
    if many:
        kg[...] = jnp.zeros_like(kg)
        vg[...] = jnp.zeros_like(vg)
    for h in range(width // HEAD_DIM):
        cols = slice(h * HEAD_DIM, (h + 1) * HEAD_DIM)

        def body(start):
            at = pl.ds(start, step)
            q, k, v = q_ref[at, cols], k_ref[:, cols], v_ref[:, cols]
            s = dot(q, k, 1, 1) * scale
            qi = lax.broadcasted_iota(jnp.int32, s.shape, 0) + start
            ki = lax.broadcasted_iota(jnp.int32, s.shape, 1)
            s = jnp.where(qi >= ki, s, -1e30)
            e = jnp.exp(s - jnp.max(s, -1, keepdims=True))
            p = e * (1.0 / jnp.sum(e, -1, keepdims=True))
            p_low = p.astype(BF16)
            attended = dot(p_low, v, 1, 0)
            later = g_ref[at, cols]
            low = later.astype(BF16)
            delta = jnp.sum(later * attended, -1, keepdims=True)
            sg = (p * (dot(low, v, 1, 1) - delta)).astype(BF16)
            a_ref[pl.ds(start + 8, step), cols] = attended
            qg[at, cols] = (dot(sg, k, 1, 0) * scale).astype(BF16).astype(F32)
            new_k = dot(sg, q, 0, 0) * scale
            new_v = dot(p_low, low, 0, 0)
            if many:
                kg[:, cols] += new_k
                vg[:, cols] += new_v
            else:
                kg[:, cols] = new_k.astype(BF16).astype(F32)
                vg[:, cols] = new_v.astype(BF16).astype(F32)

        if many:

            def run(i, carry):
                body(pl.multiple_of(i * step, step))
                return carry

            lax.fori_loop(0, length // step, run, 0)
        else:
            body(0)
    if many:
        kg[...] = kg[...].astype(BF16).astype(F32)
        vg[...] = vg[...].astype(BF16).astype(F32)
    for t, ref in enumerate((qg, kg, vg)):
        for i in range(n):
            outs[i][t * rc : (t + 1) * rc, :] = ref[aligned(goal[i], rc), :].astype(BF16)
        for j in range(POOL):
            wg_ref[t * POOL + j, :] = jnp.sum(ref[...] * x_ref[j].astype(F32), 0)
    shifted = a_ref[7 : length + 7, :].astype(BF16).astype(F32)
    for j in range(POOL):
        wg_ref[3 * POOL + j, :] = jnp.sum(shifted * y_ref[j].astype(F32), 0)
    low = wg_ref[...].astype(BF16)
    for i in range(n):
        outs[i][3 * rc :, :] = low


def collect_kernel(n, nd, wide, *refs):
    blocks, outs, held = refs[: -nd - 1], refs[-nd - 1 : -1], refs[-1]
    place, col, share = places(n), lax.axis_index("dp"), n // nd
    cw = blocks[0].shape[1]
    for c in range(len(blocks) // n):
        for i in range(n):
            part = blocks[c * n + i][...].astype(F32)
            cols = pl.ds(pl.multiple_of(lax.rem(place[i], share) * wide + c * cw, HEAD_DIM), cw)
            for t in range(KINDS):
                held[lax.div(place[i], share), t, :, cols] = part[t * POOL : (t + 1) * POOL]
    for k in range(nd):
        outs[k][...] = held[lax.bitwise_xor(col, jnp.int32(k))]


def spread_kernel(n, nd, wide, weight, *refs):
    blocks, out = refs[:-1], refs[-1]
    place, col, share = places(n), lax.axis_index("dp"), n // nd
    rc = out.shape[0] // POOL
    cw = blocks[0].shape[1]
    sel = interleave_matrix(rc * POOL)
    for c in range(len(blocks) // n):
        for i in range(n):
            ref = blocks[c * n + i]
            cols = pl.ds(pl.multiple_of(place[i] * wide + c * cw, HEAD_DIM), cw)
            w = weight[
                lax.bitwise_xor(col, lax.div(place[i], share)),
                :,
                pl.ds(pl.multiple_of(lax.rem(place[i], share) * wide + c * cw, HEAD_DIM), cw),
            ]
            parts = [ref[t * rc : (t + 1) * rc, :].astype(F32) for t in range(3)]
            made = []
            for j in range(POOL):
                total = parts[0] * w[j][None, :]
                for t in range(1, 3):
                    total = total + parts[t] * w[t * POOL + j][None, :]
                made.append(total.astype(BF16))
            out[:, cols] = dot(sel, jnp.concatenate(made, 0), 0, 0).astype(BF16)


def per_device(n, nd, block_input, cotangent, pool_weight):
    inputs = block_input[0]
    upstream = cotangent[0]
    rows, width = inputs.shape
    wide = width // n
    rc = rows // POOL
    length = rc * n
    heads = wide // HEAD_DIM
    chunks = CHUNKS if heads % CHUNKS == 0 else 1
    cw = wide // chunks
    todo = messages(n)
    shape = jax.ShapeDtypeStruct

    arrived = []
    for c in range(chunks):
        cut = pl.pallas_call(
            functools.partial(cut_kernel, n, wide, c * cw),
            out_shape=[shape((2 * rows, cw), BF16)] * n,
            in_specs=[ANY, ANY],
            out_specs=[VMEM] * n,
            scratch_shapes=[pltpu.SemaphoreType.DMA((2 * n,))],
        )(inputs, upstream)
        got = [cut[0]]
        for b, m in zip(cut[1:], todo):
            got.append(send(b, "seq", n, m))
        arrived.append(got)
    own = pool_weight.reshape(KINDS * POOL, -1)
    pieces = [own] + [send(own, "dp", nd, k) for k in range(1, nd)]
    weights = jnp.stack(pieces)

    back = []
    for c in range(chunks):
        full = lambda kind: pltpu.VMEM((length, cw), kind)
        made = pl.pallas_call(
            functools.partial(block_kernel, n, nd, rc, wide, c * cw),
            out_shape=[shape((3 * rc + KINDS * POOL, cw), BF16)] * n,
            in_specs=[VMEM] * (1 + n),
            out_specs=[VMEM] * n,
            scratch_shapes=[full(BF16)] * 3
            + [pltpu.VMEM((POOL, length, cw), BF16)] * 2
            + [pltpu.VMEM((length + 8, cw), F32)] * 2
            + [full(F32)] * 3
            + [pltpu.VMEM((KINDS * POOL, cw), F32)],
        )(weights, *arrived[c])
        back += [made[0]] + [send(b, "seq", n, m) for b, m in zip(made[1:], todo)]

    tail = pl.BlockSpec((KINDS * POOL, cw), lambda i: (3 * rc // (KINDS * POOL), 0))
    owned = (KINDS, POOL, width // nd)
    part = pl.BlockSpec(owned, lambda i: (0, 0, 0))
    shares = pl.pallas_call(
        functools.partial(collect_kernel, n, nd, wide),
        out_shape=[shape(owned, F32)] * nd,
        grid=(1,),
        in_specs=[tail] * len(back),
        out_specs=[part] * nd,
        scratch_shapes=[pltpu.VMEM((nd,) + owned, F32)],
    )(*back)
    weight_grad = shares[0]
    for k in range(1, nd):
        weight_grad = weight_grad + send(shares[k], "dp", nd, k)
    input_grad = pl.pallas_call(
        functools.partial(spread_kernel, n, nd, wide),
        out_shape=shape((rows, width), BF16),
        in_specs=[VMEM] * (1 + len(back)),
        out_specs=VMEM,
    )(weights, *back)
    return input_grad[None], weight_grad


def solution(mesh):
    n, nd = mesh.shape["seq"], mesh.shape["dp"]
    if n < 4 or n & (n - 1) or n % nd:
        raise ValueError("unsupported mesh")
    placed = (P("dp", "seq", None), P("dp", "seq", None), P(None, None, "dp"))

    def whole_step(*arrays):
        return per_device(n, nd, *arrays)

    return jax.shard_map(
        whole_step,
        mesh=mesh,
        in_specs=placed,
        out_specs=(P("dp", "seq", None), P(None, None, "dp")),
        check_vma=False,
    )
```

```python
import functools

import jax
import jax.numpy as jnp
from jax import lax
from jax.experimental import pallas as pl
from jax.experimental.pallas import tpu as pltpu
from jax.sharding import PartitionSpec as P


HEAD_DIM = 128
POOL = 4
KINDS = 4
CHUNKS = 2
BF16 = jnp.bfloat16
F32 = jnp.float32


VMEM = pl.BlockSpec(memory_space=pltpu.VMEM)
ANY = pl.BlockSpec(memory_space=pl.ANY)


def dot(a, b, ca, cb):
    return lax.dot_general(a, b, (((ca,), (cb,)), ((), ())), preferred_element_type=F32)


def messages(n):
    return [*range(n // 2, n), *range(2, n // 2), 1]


def send(block, axis, n, message):
    return lax.ppermute(block, axis, [(s, s ^ message) for s in range(n)])


def places(n):
    me = lax.axis_index("seq")
    return [me] + [lax.bitwise_xor(me, jnp.int32(m)) for m in messages(n)]


def interleave_matrix(rows):
    r = lax.broadcasted_iota(jnp.int32, (rows, rows), 0)
    t = lax.broadcasted_iota(jnp.int32, (rows, rows), 1)
    hit = t == POOL * r
    for j in range(1, POOL):
        hit = hit | (t - j == POOL * r - j * rows)
    return jnp.where(hit, 1.0, 0.0).astype(BF16)


def aligned(index, size):
    return pl.ds(pl.multiple_of(index * size, size), size)


def cut_kernel(n, wide, first, which, x_ref, y_ref, *refs):
    outs, sem = refs[:-1], refs[-1]
    rows = x_ref.shape[0]
    cw = outs[0].shape[1]
    copies = []
    goal = [places(n)[i] for i in which]
    for i in range(len(which)):
        cols = pl.ds(pl.multiple_of(goal[i] * wide + first, HEAD_DIM), cw)
        for t, ref in enumerate((x_ref, y_ref)):
            copy = pltpu.make_async_copy(ref.at[:, cols], outs[i].at[t * rows : (t + 1) * rows, :], sem.at[2 * i + t])
            copy.start()
            copies.append(copy)
    for copy in copies:
        copy.wait()


def block_kernel(n, nd, rc, wide, first, weight, *refs):
    blocks = refs[:n]
    outs = refs[n : 2 * n]
    q_ref, k_ref, v_ref, x_ref, y_ref, g_ref, a_ref, qg, kg, vg, wg_ref = refs[2 * n :]
    length, width = q_ref.shape
    rows = rc * POOL
    place = places(n)
    goal = place
    me, col, share = lax.axis_index("seq"), lax.axis_index("dp"), n // nd
    w = weight[
        lax.bitwise_xor(col, lax.div(me, share)),
        :,
        pl.ds(pl.multiple_of(lax.rem(me, share) * wide + first, HEAD_DIM), width),
    ]
    sel = interleave_matrix(rows)
    for i in range(n):
        at = aligned(place[i], rc)
        x = dot(sel, blocks[i][:rows, :], 1, 0)
        y = dot(sel, blocks[i][rows:, :], 1, 0)
        for j in range(POOL):
            x_ref[j, at, :] = x[j * rc : (j + 1) * rc].astype(BF16)
            y_ref[j, at, :] = y[j * rc : (j + 1) * rc].astype(BF16)
        for t, (ref, src) in enumerate(((q_ref, x), (k_ref, x), (v_ref, x), (g_ref, y))):
            total = src[:rc] * w[t * POOL][None, :]
            for j in range(1, POOL):
                total = total + src[j * rc : (j + 1) * rc] * w[t * POOL + j][None, :]
            ref[at, :] = total.astype(BF16).astype(ref.dtype)
    g_ref[length:, :] = jnp.zeros((8, width), F32)
    g_ref[:length, :] = g_ref[1 : length + 1, :]
    a_ref[:8, :] = jnp.zeros((8, width), F32)
    scale = HEAD_DIM**-0.5
    step = min(length, 256)
    many = length > step
    if many:
        kg[...] = jnp.zeros_like(kg)
        vg[...] = jnp.zeros_like(vg)
    for h in range(width // HEAD_DIM):
        cols = slice(h * HEAD_DIM, (h + 1) * HEAD_DIM)

        def body(start):
            at = pl.ds(start, step)
            q, k, v = q_ref[at, cols], k_ref[:, cols], v_ref[:, cols]
            s = dot(q, k, 1, 1) * scale
            qi = lax.broadcasted_iota(jnp.int32, s.shape, 0) + start
            ki = lax.broadcasted_iota(jnp.int32, s.shape, 1)
            s = jnp.where(qi >= ki, s, -1e30)
            e = jnp.exp(s - jnp.max(s, -1, keepdims=True))
            p = e * (1.0 / jnp.sum(e, -1, keepdims=True))
            p_low = p.astype(BF16)
            attended = dot(p_low, v, 1, 0)
            later = g_ref[at, cols]
            low = later.astype(BF16)
            delta = jnp.sum(later * attended, -1, keepdims=True)
            sg = (p * (dot(low, v, 1, 1) - delta)).astype(BF16)
            a_ref[pl.ds(start + 8, step), cols] = attended
            qg[at, cols] = (dot(sg, k, 1, 0) * scale).astype(BF16).astype(F32)
            new_k = dot(sg, q, 0, 0) * scale
            new_v = dot(p_low, low, 0, 0)
            if many:
                kg[:, cols] += new_k
                vg[:, cols] += new_v
            else:
                kg[:, cols] = new_k.astype(BF16).astype(F32)
                vg[:, cols] = new_v.astype(BF16).astype(F32)

        if many:

            def run(i, carry):
                body(pl.multiple_of(i * step, step))
                return carry

            lax.fori_loop(0, length // step, run, 0)
        else:
            body(0)
    if many:
        kg[...] = kg[...].astype(BF16).astype(F32)
        vg[...] = vg[...].astype(BF16).astype(F32)
    for t, ref in enumerate((qg, kg, vg)):
        for i in range(n):
            outs[i][t * rc : (t + 1) * rc, :] = ref[aligned(goal[i], rc), :].astype(BF16)
        for j in range(POOL):
            wg_ref[t * POOL + j, :] = jnp.sum(ref[...] * x_ref[j].astype(F32), 0)
    shifted = a_ref[7 : length + 7, :].astype(BF16).astype(F32)
    for j in range(POOL):
        wg_ref[3 * POOL + j, :] = jnp.sum(shifted * y_ref[j].astype(F32), 0)
    low = wg_ref[...].astype(BF16)
    for i in range(n):
        outs[i][3 * rc :, :] = low


def collect_kernel(n, nd, wide, *refs):
    blocks, outs, held = refs[: -nd - 1], refs[-nd - 1 : -1], refs[-1]
    place, col, share = places(n), lax.axis_index("dp"), n // nd
    cw = blocks[0].shape[1]
    for c in range(len(blocks) // n):
        for i in range(n):
            part = blocks[c * n + i][...].astype(F32)
            cols = pl.ds(pl.multiple_of(lax.rem(place[i], share) * wide + c * cw, HEAD_DIM), cw)
            for t in range(KINDS):
                held[lax.div(place[i], share), t, :, cols] = part[t * POOL : (t + 1) * POOL]
    for k in range(nd):
        outs[k][...] = held[lax.bitwise_xor(col, jnp.int32(k))]


def spread_kernel(n, nd, wide, weight, *refs):
    blocks, out = refs[:-1], refs[-1]
    place, col, share = places(n), lax.axis_index("dp"), n // nd
    rc = out.shape[0] // POOL
    cw = blocks[0].shape[1]
    sel = interleave_matrix(rc * POOL)
    for c in range(len(blocks) // n):
        for i in range(n):
            ref = blocks[c * n + i]
            cols = pl.ds(pl.multiple_of(place[i] * wide + c * cw, HEAD_DIM), cw)
            w = weight[
                lax.bitwise_xor(col, lax.div(place[i], share)),
                :,
                pl.ds(pl.multiple_of(lax.rem(place[i], share) * wide + c * cw, HEAD_DIM), cw),
            ]
            parts = [ref[t * rc : (t + 1) * rc, :].astype(F32) for t in range(3)]
            made = []
            for j in range(POOL):
                total = parts[0] * w[j][None, :]
                for t in range(1, 3):
                    total = total + parts[t] * w[t * POOL + j][None, :]
                made.append(total.astype(BF16))
            out[:, cols] = dot(sel, jnp.concatenate(made, 0), 0, 0).astype(BF16)


def per_device(n, nd, block_input, cotangent, pool_weight):
    inputs = block_input[0]
    upstream = cotangent[0]
    rows, width = inputs.shape
    wide = width // n
    rc = rows // POOL
    length = rc * n
    heads = wide // HEAD_DIM
    chunks = CHUNKS if heads % CHUNKS == 0 else 1
    cw = wide // chunks
    todo = messages(n)
    shape = jax.ShapeDtypeStruct

    arrived = []
    for c in range(chunks):
        cut = [None] * n
        groups = [range(1, 1 + n // 2), [0, *range(1 + n // 2, n)]] if c == 0 else [range(n)]
        for part, which in enumerate(groups):
            made = pl.pallas_call(
                functools.partial(cut_kernel, n, wide, c * cw, which),
                out_shape=[shape((2 * rows, cw), BF16)] * len(which),
                in_specs=[ANY, ANY],
                out_specs=[VMEM] * len(which),
                scratch_shapes=[pltpu.SemaphoreType.DMA((2 * len(which),))],
            )(inputs, upstream)
            for i, block in zip(which, made):
                cut[i] = block
        got = [cut[0]]
        for b, m in zip(cut[1:], todo):
            got.append(send(b, "seq", n, m))
        arrived.append(got)
    own = pool_weight.reshape(KINDS * POOL, -1)
    pieces = [own] + [send(own, "dp", nd, k) for k in range(1, nd)]
    weights = jnp.stack(pieces)

    back = []
    for c in range(chunks):
        full = lambda kind: pltpu.VMEM((length, cw), kind)
        made = pl.pallas_call(
            functools.partial(block_kernel, n, nd, rc, wide, c * cw),
            out_shape=[shape((3 * rc + KINDS * POOL, cw), BF16)] * n,
            in_specs=[VMEM] * (1 + n),
            out_specs=[VMEM] * n,
            scratch_shapes=[full(BF16)] * 3
            + [pltpu.VMEM((POOL, length, cw), BF16)] * 2
            + [pltpu.VMEM((length + 8, cw), F32)] * 2
            + [full(F32)] * 3
            + [pltpu.VMEM((KINDS * POOL, cw), F32)],
        )(weights, *arrived[c])
        back.append(made[0])
        for b, m in zip(made[1:], todo):
            back.append(send(b, "seq", n, m))

    tail = pl.BlockSpec((KINDS * POOL, cw), lambda i: (3 * rc // (KINDS * POOL), 0))
    owned = (KINDS, POOL, width // nd)
    part = pl.BlockSpec(owned, lambda i: (0, 0, 0))
    shares = pl.pallas_call(
        functools.partial(collect_kernel, n, nd, wide),
        out_shape=[shape(owned, F32)] * nd,
        grid=(1,),
        in_specs=[tail] * len(back),
        out_specs=[part] * nd,
        scratch_shapes=[pltpu.VMEM((nd,) + owned, F32)],
    )(*back)
    weight_grad = shares[0]
    for k in range(1, nd):
        weight_grad = weight_grad + send(shares[k], "dp", nd, k)
    input_grad = pl.pallas_call(
        functools.partial(spread_kernel, n, nd, wide),
        out_shape=shape((rows, width), BF16),
        in_specs=[VMEM] * (1 + len(back)),
        out_specs=VMEM,
    )(weights, *back)
    return input_grad[None], weight_grad


def solution(mesh):
    n, nd = mesh.shape["seq"], mesh.shape["dp"]
    if n < 4 or n & (n - 1) or n % nd:
        raise ValueError("unsupported mesh")
    placed = (P("dp", "seq", None), P("dp", "seq", None), P(None, None, "dp"))

    def whole_step(*arrays):
        return per_device(n, nd, *arrays)

    return jax.shard_map(
        whole_step,
        mesh=mesh,
        in_specs=placed,
        out_specs=(P("dp", "seq", None), P(None, None, "dp")),
        check_vma=False,
    )
```

```python
import functools

import jax
import jax.numpy as jnp
from jax import lax
from jax.experimental import pallas as pl
from jax.experimental.pallas import tpu as pltpu
from jax.sharding import PartitionSpec as P


HEAD_DIM = 128
POOL = 4
KINDS = 4
CHUNKS = 2
BF16 = jnp.bfloat16
F32 = jnp.float32


VMEM = pl.BlockSpec(memory_space=pltpu.VMEM)
ANY = pl.BlockSpec(memory_space=pl.ANY)


def dot(a, b, ca, cb):
    return lax.dot_general(a, b, (((ca,), (cb,)), ((), ())), preferred_element_type=F32)


def messages(n):
    return [*range(n // 2, n), *range(2, n // 2), 1]


def send(block, axis, n, message):
    return lax.ppermute(block, axis, [(s, s ^ message) for s in range(n)])


def places(n):
    me = lax.axis_index("seq")
    return [me] + [lax.bitwise_xor(me, jnp.int32(m)) for m in messages(n)]


def interleave_matrix(rows):
    r = lax.broadcasted_iota(jnp.int32, (rows, rows), 0)
    t = lax.broadcasted_iota(jnp.int32, (rows, rows), 1)
    hit = t == POOL * r
    for j in range(1, POOL):
        hit = hit | (t - j == POOL * r - j * rows)
    return jnp.where(hit, 1.0, 0.0).astype(BF16)


def aligned(index, size):
    return pl.ds(pl.multiple_of(index * size, size), size)


def cut_kernel(n, wide, first, which, x_ref, y_ref, *refs):
    outs, sem = refs[:-1], refs[-1]
    rows = x_ref.shape[0]
    cw = outs[0].shape[1]
    copies = []
    goal = [places(n)[i] for i in which]
    for i in range(len(which)):
        cols = pl.ds(pl.multiple_of(goal[i] * wide + first, HEAD_DIM), cw)
        for t, ref in enumerate((x_ref, y_ref)):
            copy = pltpu.make_async_copy(ref.at[:, cols], outs[i].at[t * rows : (t + 1) * rows, :], sem.at[2 * i + t])
            copy.start()
            copies.append(copy)
    for copy in copies:
        copy.wait()


def block_kernel(n, nd, rc, wide, first, weight, *refs):
    blocks = refs[:n]
    outs = refs[n : 2 * n]
    q_ref, k_ref, v_ref, x_ref, y_ref, g_ref, a_ref, qg, kg, vg, wg_ref = refs[2 * n :]
    length, width = q_ref.shape
    rows = rc * POOL
    place = places(n)
    goal = place
    me, col, share = lax.axis_index("seq"), lax.axis_index("dp"), n // nd
    w = weight[
        lax.bitwise_xor(col, lax.div(me, share)),
        :,
        pl.ds(pl.multiple_of(lax.rem(me, share) * wide + first, HEAD_DIM), width),
    ]
    sel = interleave_matrix(rows)
    for i in range(n):
        at = aligned(place[i], rc)
        x = dot(sel, blocks[i][:rows, :], 1, 0)
        y = dot(sel, blocks[i][rows:, :], 1, 0)
        for j in range(POOL):
            x_ref[j, at, :] = x[j * rc : (j + 1) * rc].astype(BF16)
            y_ref[j, at, :] = y[j * rc : (j + 1) * rc].astype(BF16)
        for t, (ref, src) in enumerate(((q_ref, x), (k_ref, x), (v_ref, x), (g_ref, y))):
            total = src[:rc] * w[t * POOL][None, :]
            for j in range(1, POOL):
                total = total + src[j * rc : (j + 1) * rc] * w[t * POOL + j][None, :]
            ref[at, :] = total.astype(BF16).astype(ref.dtype)
    g_ref[length:, :] = jnp.zeros((8, width), F32)
    g_ref[:length, :] = g_ref[1 : length + 1, :]
    a_ref[:8, :] = jnp.zeros((8, width), F32)
    scale = HEAD_DIM**-0.5
    step = min(length, 256)
    many = length > step
    if many:
        kg[...] = jnp.zeros_like(kg)
        vg[...] = jnp.zeros_like(vg)
    for h in range(width // HEAD_DIM):
        cols = slice(h * HEAD_DIM, (h + 1) * HEAD_DIM)

        def body(start):
            at = pl.ds(start, step)
            q, k, v = q_ref[at, cols], k_ref[:, cols], v_ref[:, cols]
            s = dot(q, k, 1, 1) * scale
            qi = lax.broadcasted_iota(jnp.int32, s.shape, 0) + start
            ki = lax.broadcasted_iota(jnp.int32, s.shape, 1)
            s = jnp.where(qi >= ki, s, -1e30)
            e = jnp.exp(s - jnp.max(s, -1, keepdims=True))
            p = e * (1.0 / jnp.sum(e, -1, keepdims=True))
            p_low = p.astype(BF16)
            attended = dot(p_low, v, 1, 0)
            later = g_ref[at, cols]
            low = later.astype(BF16)
            delta = jnp.sum(later * attended, -1, keepdims=True)
            sg = (p * (dot(low, v, 1, 1) - delta)).astype(BF16)
            a_ref[pl.ds(start + 8, step), cols] = attended
            qg[at, cols] = (dot(sg, k, 1, 0) * scale).astype(BF16).astype(F32)
            new_k = dot(sg, q, 0, 0) * scale
            new_v = dot(p_low, low, 0, 0)
            if many:
                kg[:, cols] += new_k
                vg[:, cols] += new_v
            else:
                kg[:, cols] = new_k.astype(BF16).astype(F32)
                vg[:, cols] = new_v.astype(BF16).astype(F32)

        if many:

            def run(i, carry):
                body(pl.multiple_of(i * step, step))
                return carry

            lax.fori_loop(0, length // step, run, 0)
        else:
            body(0)
    if many:
        kg[...] = kg[...].astype(BF16).astype(F32)
        vg[...] = vg[...].astype(BF16).astype(F32)
    for t, ref in enumerate((qg, kg, vg)):
        for i in range(n):
            outs[i][t * rc : (t + 1) * rc, :] = ref[aligned(goal[i], rc), :].astype(BF16)
        for j in range(POOL):
            wg_ref[t * POOL + j, :] = jnp.sum(ref[...] * x_ref[j].astype(F32), 0)
    shifted = a_ref[7 : length + 7, :].astype(BF16).astype(F32)
    for j in range(POOL):
        wg_ref[3 * POOL + j, :] = jnp.sum(shifted * y_ref[j].astype(F32), 0)
    low = wg_ref[...].astype(BF16)
    for i in range(n):
        outs[i][3 * rc :, :] = low


def collect_kernel(n, nd, wide, *refs):
    blocks, outs, held = refs[: -nd - 1], refs[-nd - 1 : -1], refs[-1]
    place, col, share = places(n), lax.axis_index("dp"), n // nd
    cw = blocks[0].shape[1]
    for c in range(len(blocks) // n):
        for i in range(n):
            part = blocks[c * n + i][...].astype(F32)
            cols = pl.ds(pl.multiple_of(lax.rem(place[i], share) * wide + c * cw, HEAD_DIM), cw)
            for t in range(KINDS):
                held[lax.div(place[i], share), t, :, cols] = part[t * POOL : (t + 1) * POOL]
    for k in range(nd):
        outs[k][...] = held[lax.bitwise_xor(col, jnp.int32(k))]


def spread_kernel(n, nd, wide, first, weight, *refs):
    blocks, (out, made_ref, sem) = refs[:n], refs[-3:]
    place, col, share = places(n), lax.axis_index("dp"), n // nd
    rows, cw = made_ref.shape[1:]
    rc = rows // POOL
    sel = interleave_matrix(rows)
    copies = []
    for i in range(n):
        ref = blocks[i]
        w = weight[
            lax.bitwise_xor(col, lax.div(place[i], share)),
            :,
            pl.ds(pl.multiple_of(lax.rem(place[i], share) * wide + first, HEAD_DIM), cw),
        ]
        parts = [ref[t * rc : (t + 1) * rc, :].astype(F32) for t in range(3)]
        made = []
        for j in range(POOL):
            total = parts[0] * w[j][None, :]
            for t in range(1, 3):
                total = total + parts[t] * w[t * POOL + j][None, :]
            made.append(total.astype(BF16))
        made_ref[i] = dot(sel, jnp.concatenate(made, 0), 0, 0).astype(BF16)
        cols = pl.ds(pl.multiple_of(place[i] * wide + first, HEAD_DIM), cw)
        copy = pltpu.make_async_copy(made_ref.at[i], out.at[:, cols], sem.at[i])
        copy.start()
        copies.append(copy)
    for copy in copies:
        copy.wait()


def per_device(n, nd, block_input, cotangent, pool_weight):
    inputs = block_input[0]
    upstream = cotangent[0]
    rows, width = inputs.shape
    wide = width // n
    rc = rows // POOL
    length = rc * n
    heads = wide // HEAD_DIM
    chunks = CHUNKS if heads % CHUNKS == 0 else 1
    cw = wide // chunks
    todo = messages(n)
    shape = jax.ShapeDtypeStruct

    arrived = []
    for c in range(chunks):
        cut = [None] * n
        groups = [range(1, 1 + n // 2), [0, *range(1 + n // 2, n)]] if c == 0 else [range(n)]
        for part, which in enumerate(groups):
            made = pl.pallas_call(
                functools.partial(cut_kernel, n, wide, c * cw, which),
                out_shape=[shape((2 * rows, cw), BF16)] * len(which),
                in_specs=[ANY, ANY],
                out_specs=[VMEM] * len(which),
                scratch_shapes=[pltpu.SemaphoreType.DMA((2 * len(which),))],
            )(inputs, upstream)
            for i, block in zip(which, made):
                cut[i] = block
        got = [cut[0]]
        for b, m in zip(cut[1:], todo):
            got.append(send(b, "seq", n, m))
        arrived.append(got)
    own = pool_weight.reshape(KINDS * POOL, -1)
    pieces = [own] + [send(own, "dp", nd, k) for k in range(1, nd)]
    weights = jnp.stack(pieces)

    back = []
    for c in range(chunks):
        full = lambda kind: pltpu.VMEM((length, cw), kind)
        made = pl.pallas_call(
            functools.partial(block_kernel, n, nd, rc, wide, c * cw),
            out_shape=[shape((3 * rc + KINDS * POOL, cw), BF16)] * n,
            in_specs=[VMEM] * (1 + n),
            out_specs=[VMEM] * n,
            scratch_shapes=[full(BF16)] * 3
            + [pltpu.VMEM((POOL, length, cw), BF16)] * 2
            + [pltpu.VMEM((length + 8, cw), F32)] * 2
            + [full(F32)] * 3
            + [pltpu.VMEM((KINDS * POOL, cw), F32)],
        )(weights, *arrived[c])
        back.append(made[0])
        for b, m in zip(made[1:], todo):
            back.append(send(b, "seq", n, m))

    tail = pl.BlockSpec((KINDS * POOL, cw), lambda i: (3 * rc // (KINDS * POOL), 0))
    owned = (KINDS, POOL, width // nd)
    part = pl.BlockSpec(owned, lambda i: (0, 0, 0))
    shares = pl.pallas_call(
        functools.partial(collect_kernel, n, nd, wide),
        out_shape=[shape(owned, F32)] * nd,
        grid=(1,),
        in_specs=[tail] * len(back),
        out_specs=[part] * nd,
        scratch_shapes=[pltpu.VMEM((nd,) + owned, F32)],
    )(*back)
    weight_grad = shares[0]
    for k in range(1, nd):
        weight_grad = weight_grad + send(shares[k], "dp", nd, k)
    input_grad = ()
    for c in range(chunks):
        input_grad = (
            pl.pallas_call(
                functools.partial(spread_kernel, n, nd, wide, c * cw),
                out_shape=shape((rows, width), BF16),
                in_specs=[VMEM] * (1 + n) + [ANY] * len(input_grad),
                out_specs=ANY,
                input_output_aliases={1 + n: 0} if input_grad else {},
                scratch_shapes=[pltpu.VMEM((n, rows, cw), BF16), pltpu.SemaphoreType.DMA((n,))],
            )(weights, *back[c * n : (c + 1) * n], *input_grad),
        )
    return input_grad[0][None], weight_grad


def solution(mesh):
    n, nd = mesh.shape["seq"], mesh.shape["dp"]
    if n < 4 or n & (n - 1) or n % nd:
        raise ValueError("unsupported mesh")
    placed = (P("dp", "seq", None), P("dp", "seq", None), P(None, None, "dp"))

    def whole_step(*arrays):
        return per_device(n, nd, *arrays)

    return jax.shard_map(
        whole_step,
        mesh=mesh,
        in_specs=placed,
        out_specs=(P("dp", "seq", None), P(None, None, "dp")),
        check_vma=False,
    )
```
